16 devices in a mesh: dp: 2 (over z), stage: 2 (over y), tp: 4 (over x, core).
Axes of the slice: x: 2, y: 2, z: 2, core: 2. Of those that a mesh axis runs over, the one named last changes fastest.
Arguments:
- act_in: bfloat16 [2, 24, 14, 14, 1024], P('stage', ('dp', 'tp'))
- w_conv: bfloat16 [2, 3, 3, 1024, 1024], P('stage', None, None, 'tp')
- w_short: bfloat16 [2, 1024, 1024], P('stage', 'tp')
- gamma: float32 [2, 1024], P('stage', 'tp')
- beta: float32 [2, 1024], P('stage', 'tp')
- gamma_s: float32 [2, 1024], P('stage', 'tp')
- grad_z: bfloat16 [2, 24, 14, 14, 1024], P('stage', 'dp', None, None, 'tp')
Outputs:
- output 1: bfloat16 [2, 24, 14, 14, 1024], P('stage', 'dp', None, None, 'tp')
- output 2: bfloat16 [2, 24, 14, 14, 1024], P('stage', ('dp', 'tp'))
- output 3: float32 [2, 3, 3, 1024, 1024], P('stage', None, None, 'tp')
- output 4: float32 [2, 1024, 1024], P('stage', 'tp')
All inputs are finite; a program needn't handle non-finite values.
Results may differ from the reference program's by a relative error of at most 0.00668.
Values are sent between devices in bfloat16 or wider.
A program may use at most 1 GiB of HBM per device.

```python
import jax
import jax.numpy as jnp
from jax import lax

NUM_STAGES = 2
BATCH_ALL = 24
BLOCK_IMGS = 3
IMG_HEIGHT = 14
IMG_WIDTH = 14
CH_IN = 1024
CH_OUT = 1024


def place_slot(array_in, slot_index):
    pad_before = jnp.zeros((slot_index,) + array_in.shape, array_in.dtype)
    pad_after = jnp.zeros((NUM_STAGES - slot_index - 1,) + array_in.shape, array_in.dtype)
    return jnp.concatenate([pad_before, array_in[None], pad_after], axis=0)


def setup_inputs(seed: int = 0) -> dict:
    key_list = jax.random.split(jax.random.key(seed), 7)
    act_draw = jax.random.normal(key_list[0], (BATCH_ALL, IMG_HEIGHT, IMG_WIDTH, CH_IN), jnp.float32)
    conv_draw = jax.random.normal(key_list[1], (3, 3, CH_IN, CH_OUT), jnp.float32) * (9 * CH_IN) ** -0.5
    short_draw = jax.random.normal(key_list[2], (CH_IN, CH_OUT), jnp.float32) * CH_IN ** -0.5
    gamma_draw = jax.random.uniform(key_list[3], (CH_OUT,), jnp.float32, 0.5, 1.5)
    beta_draw = 0.5 * jax.random.normal(key_list[4], (CH_OUT,), jnp.float32)
    gamma_s_draw = jax.random.uniform(key_list[5], (CH_OUT,), jnp.float32, 0.5, 1.5)
    grad_draw = jax.random.normal(key_list[6], (BATCH_ALL, IMG_HEIGHT, IMG_WIDTH, CH_OUT), jnp.float32)
    return {
        "act_in": place_slot(act_draw.astype(jnp.bfloat16), 0),
        "w_conv": place_slot(conv_draw.astype(jnp.bfloat16), 1),
        "w_short": place_slot(short_draw.astype(jnp.bfloat16), 1),
        "gamma": place_slot(gamma_draw, 1),
        "beta": place_slot(beta_draw, 1),
        "gamma_s": place_slot(gamma_s_draw, 1),
        "grad_z": place_slot(grad_draw.astype(jnp.bfloat16), 1),
    }


def reference(act_in, w_conv, w_short, gamma, beta, gamma_s, grad_z):
    kernel = w_conv[1].astype(jnp.float32)
    short_w = w_short[1].astype(jnp.float32)
    scale_main = gamma[1]
    shift_main = beta[1]
    scale_short = gamma_s[1]
    num_blocks = BATCH_ALL // BLOCK_IMGS
    act_blocks = act_in[0].reshape(num_blocks, BLOCK_IMGS, IMG_HEIGHT, IMG_WIDTH, CH_IN)
    grad_blocks = grad_z[1].reshape(num_blocks, BLOCK_IMGS, IMG_HEIGHT, IMG_WIDTH, CH_OUT)

    def linear_part(images, conv_w, proj_w):
        pre_act = lax.conv_general_dilated(images, conv_w, (1, 1), "SAME", dimension_numbers=("NHWC", "HWIO", "NHWC"))
        short_out = jnp.einsum("nhwc,co->nhwo", images, proj_w)
        return pre_act, short_out

    def block_step(acc_pair, block_in):
        act_blk, grad_blk = block_in
        (pre_act, short_out), pull_back = jax.vjp(linear_part, act_blk.astype(jnp.float32), kernel, short_w)
        mixed_sum = pre_act * scale_main + shift_main + short_out * scale_short
        z_blk = jnp.maximum(mixed_sum, 0.0).astype(jnp.bfloat16)
        mask_pos = mixed_sum > 0.0
        grad_wide = grad_blk.astype(jnp.float32)
        g_main = jnp.where(mask_pos, grad_wide * scale_main, 0.0).astype(jnp.bfloat16)
        g_short = jnp.where(mask_pos, grad_wide * scale_short, 0.0).astype(jnp.bfloat16)
        grad_images, grad_conv, grad_proj = pull_back((g_main.astype(jnp.float32), g_short.astype(jnp.float32)))
        new_acc = (acc_pair[0] + grad_conv, acc_pair[1] + grad_proj)
        return new_acc, (z_blk, grad_images.astype(jnp.bfloat16))

    acc_init = (jnp.zeros((3, 3, CH_IN, CH_OUT), jnp.float32), jnp.zeros((CH_IN, CH_OUT), jnp.float32))
    (dw_sum, dws_sum), (z_blocks, dx_blocks) = lax.scan(block_step, acc_init, (act_blocks, grad_blocks))
    z_all = z_blocks.reshape(BATCH_ALL, IMG_HEIGHT, IMG_WIDTH, CH_OUT)
    dx_all = dx_blocks.reshape(BATCH_ALL, IMG_HEIGHT, IMG_WIDTH, CH_IN)
    return (place_slot(z_all, 1), place_slot(dx_all, 0), place_slot(dw_sum, 1), place_slot(dws_sum, 1))
```

```python
import jax
import jax.numpy as jnp
from jax import lax
from jax.experimental import pallas as pl
from jax.experimental.pallas import tpu as pltpu
from jax.sharding import PartitionSpec as P

BF = jnp.bfloat16
F32 = jnp.float32
MESH = pl.DeviceIdType.MESH
ROWS = 224
HALO = 240
SET = 4 * ROWS
NT = (((1,), (1,)), ((), ()))


def dot(a, b):
    return jnp.dot(a, b, preferred_element_type=F32)


def dot_t(a, b):
    return lax.dot_general(a, b, NT, preferred_element_type=F32)


def mo(v, m):
    return pl.multiple_of(v, m)


def block_kernel(
    x0, wc, ws, vec, dz_in,
    z_out, dx_out, dw_out, ds_out,
    xa, wo, wr, vecs, dz, ga, xz, xt, gh, gsh, gx, gsx, dwa, zs, dxs,
    s_send, s_loc, r_ws, r_wx, r_wz, r_v, r_x, r_xz, r_g, r_dx,
):
    z = lax.axis_index("dp")
    st = lax.axis_index("stage")
    k = lax.axis_index("tp")
    zo = 1 - z
    k1 = k + 1 - 2 * lax.rem(k, 2)
    k2 = lax.rem(k + 2, 4)
    k3 = 3 - k

    def dev(dp=None, stage=None, tp=None):
        return (z if dp is None else dp, st if stage is None else stage, k if tp is None else tp)

    sends = []

    def send(src, dst, rsem, **to):
        c = pltpu.make_async_remote_copy(src, dst, s_send.at[len(sends)], rsem, device_id=dev(**to), device_id_type=MESH)
        c.start()
        sends.append(c)

    def recv(dst, rsem):
        pltpu.make_async_remote_copy(dst, dst, s_send.at[0], rsem, device_id=dev(), device_id_type=MESH).wait_recv()

    def image(n):
        return xa.at[pl.ds(mo((n * 15 + 1) * 16, 16), ROWS)]

    @pl.when(st == 0)
    def _():
        for i in range(3):
            send(x0.at[pl.ds(i * ROWS, ROWS)], image(i * 4 + k), r_x.at[i * 4 + k], tp=k2)
        for i in range(3):
            send(x0.at[pl.ds(i * ROWS, ROWS)], image(i * 4 + k), r_x.at[i * 4 + k], stage=1)
            recv(image(i * 4 + k2), r_x.at[i * 4 + k2])
            send(image(i * 4 + k2), image(i * 4 + k2), r_x.at[i * 4 + k2], stage=1)
        for i in range(3):
            for q in range(4):
                recv(dx_out.at[pl.ds(i * ROWS, ROWS), pl.ds(q * 256, 256)], r_dx.at[i, q])
        for c in sends:
            c.wait_send()

    sends.clear()

    @pl.when(st == 1)
    def _():
        kc = mo(k * 256, 256)

        def wsrc(tap, q):
            return wo.at[tap, :, pl.ds(mo(q * 256, 256), 256)]

        def wdst(tap, q):
            return wr.at[tap, pl.ds(mo(q * 256, 256), 256)]

        local = [
            pltpu.make_async_copy(wc, wo.at[pl.ds(0, 9)], s_loc.at[4]),
            pltpu.make_async_copy(ws, wo.at[9], s_loc.at[5]),
            pltpu.make_async_copy(vec, vecs.at[k], s_loc.at[2]),
            pltpu.make_async_copy(dz_in, dz, s_loc.at[3]),
            pltpu.make_async_copy(wc.at[:, :, pl.ds(kc, 256)], wr.at[pl.ds(0, 9), pl.ds(kc, 256)], s_loc.at[0]),
            pltpu.make_async_copy(ws.at[:, pl.ds(kc, 256)], wr.at[9, pl.ds(kc, 256)], s_loc.at[1]),
        ]
        for c in local:
            c.start()
        for c in local[:2]:
            c.wait()
        mine, other = z * 5, zo * 5
        for t in range(5):
            send(wsrc(mine + t, k2), wdst(mine + t, k), r_wx.at[0, t], tp=k2)
            send(wsrc(mine + t, k3), wdst(mine + t, k), r_wx.at[1, t], tp=k3)
        send(
            wo.at[:, :, pl.ds(mo(k1 * 256, 256), 256)], wr.at[:, pl.ds(kc, 256)], r_ws.at[0], tp=k1
        )
        for n, p in enumerate((k1, k2, k3)):
            send(vec, vecs.at[k], r_v.at[n], tp=p)

        def zero_rows(n, _):
            xa[pl.ds(mo(n * HALO, 16), 16)] = jnp.zeros((16, 1024), BF)
            return 0

        lax.fori_loop(0, 13, zero_rows, 0)
        for n in range(5):
            gx[pl.ds(n * HALO, 16)] = jnp.zeros((16, 1024), BF)
        for n in range(9):
            gh[pl.ds(n * HALO, 16)] = jnp.zeros((16, 256), BF)

        for t in range(5):
            for s, q in ((0, k2), (1, k3)):
                recv(wdst(mine + t, q), r_wx.at[s, t])
                send(wdst(mine + t, q), wdst(mine + t, q), r_wz.at[s, t], dp=zo)

        for n, p in enumerate((k1, k2, k3)):
            recv(vecs.at[p], r_v.at[n])
        for c in local[2:]:
            c.wait()

        def rows_of(b):
            return [mo((b * 2 + n) * HALO, 16) for n in range(2)]

        def fwd(i):
            gam, bet, gsc = vecs[k, 0:1, :], vecs[k, 1:2, :], vecs[k, 2:3, :]

            def body(b, _):
                bases = rows_of(i * 2 + b)

                def lhs(t):
                    return jnp.concatenate([xa[pl.ds(mo(s + t * 16, 16), ROWS)] for s in bases], axis=0)

                parts = []
                for j in range(3):
                    acc = dot(lhs(0), wr[j])
                    acc += dot(lhs(1), wr[3 + j])
                    acc += dot(lhs(2), wr[6 + j])
                    parts.append(acc)
                pre = parts[1] + pltpu.roll(parts[0], 1, 0) + pltpu.roll(parts[2], 447, 0)
                u = pre * gam + bet + dot(lhs(1), wr[9]) * gsc
                at = pl.ds(mo(i * SET + b * 448, 64), 448)
                zs[at] = jnp.maximum(u, 0.0).astype(BF)
                ga[z, k, at] = jnp.where(u > 0.0, dz[at].astype(F32), 0.0).astype(BF)
                return 0

            lax.fori_loop(0, 2, body, 0)

        def blk(zz, q, i):
            return ga.at[zz, q, pl.ds(i * SET, SET)]

        def gsend(zz, q, i, **to):
            send(blk(zz, q, i), blk(zz, q, i), r_g.at[zz, q, i], **to)

        def grecv(zz, q, i):
            recv(blk(zz, q, i), r_g.at[zz, q, i])

        def put_xt(val, t):
            v = val.astype(F32)
            for j in range(3):
                w = v if j == 1 else pltpu.roll(v, (1 - j) % SET, 0)
                xt[j, :, pl.ds(t * SET, SET)] = w.T.astype(BF)

        def dx(i):
            for q in range(4):
                gam, gsc = vecs[q, 0:1, :], vecs[q, 2:3, :]

                def scale(n, _):
                    v = ga[z, q, pl.ds(mo(i * SET + n * ROWS, 32), ROWS)].astype(F32)
                    gx[pl.ds(mo(n * HALO + 16, 16), ROWS), pl.ds(q * 256, 256)] = (v * gam).astype(BF)
                    gsx[pl.ds(mo(n * ROWS, 32), ROWS), pl.ds(q * 256, 256)] = (v * gsc).astype(BF)
                    return 0

                lax.fori_loop(0, 4, scale, 0)

            def body(b, _):
                bases = rows_of(b)

                def lhs(t):
                    return jnp.concatenate([gx[pl.ds(mo(s + (2 - t) * 16, 16), ROWS)] for s in bases], axis=0)

                parts = []
                for j in range(3):
                    acc = dot_t(lhs(0), wo[j])
                    acc += dot_t(lhs(1), wo[3 + j])
                    acc += dot_t(lhs(2), wo[6 + j])
                    parts.append(acc)
                tot = parts[1] + pltpu.roll(parts[0], 447, 0) + pltpu.roll(parts[2], 1, 0)
                tot += dot_t(gsx[pl.ds(mo(b * 448, 64), 448)], wo[9])
                dxs[pl.ds(mo(i * SET + b * 448, 64), 448)] = tot.astype(BF)
                return 0

            lax.fori_loop(0, 2, body, 0)
            for j in range(4):
                send(
                    dxs.at[pl.ds(i * SET + j * ROWS, ROWS)],
                    dx_out.at[pl.ds(i * ROWS, ROWS), pl.ds(kc, 256)],
                    r_dx.at[i, k],
                    stage=0, tp=j,
                )

        def dw(u, first, last):
            def per_q(q, _):
                gam, gsc = vecs[q, 0:1, :], vecs[q, 2:3, :]
                qc = pl.ds(mo(q * 256, 256), 256)

                def scale(n, _):
                    t = u * 8 + n
                    zz = jnp.where(t < 12, z, zo)
                    v = ga[zz, q, pl.ds(mo(lax.rem(t, 12) * ROWS, 32), ROWS)].astype(F32)
                    gh[pl.ds(mo(n * HALO + 16, 16), ROWS)] = (v * gam).astype(BF)
                    gsh[pl.ds(mo(n * ROWS, 32), ROWS)] = (v * gsc).astype(BF)
                    return 0

                lax.fori_loop(0, 8, scale, 0)
                lanes = pl.ds(u * 1792, 1792)
                for i in range(3):
                    rhs = jnp.concatenate([gh[pl.ds(n * HALO + (2 - i) * 16, ROWS)] for n in range(8)], axis=0)
                    for j in range(3):
                        d = dot(xt[j, :, lanes], rhs)
                        if first:
                            dwa[3 * i + j, :, qc] = d
                        else:
                            dwa[3 * i + j, :, qc] += d
                d = dot(xt[1, :, lanes], gsh[...])
                if first:
                    dwa[9, :, qc] = d
                else:
                    dwa[9, :, qc] += d
                if last:
                    pltpu.make_async_copy(dwa.at[pl.ds(0, 9), :, qc], dw_out.at[:, :, qc], s_loc.at[6 + q]).start()
                    pltpu.make_async_copy(dwa.at[9, :, qc], ds_out.at[:, qc], s_loc.at[10 + q]).start()
                return 0

            lax.fori_loop(0, 4, per_q, 0)

        def relay(i):
            grecv(z, k2, i)
            gsend(z, k2, i, tp=k1)
            grecv(zo, k, i)
            gsend(zo, k, i, tp=k2)
            gsend(zo, k, i, tp=k1)

        def backward(i):
            relay(i)
            grecv(z, k1, i)
            grecv(z, k3, i)
            dx(i)

        for i in range(3):
            for p in (k, k2):
                recv(image(i * 4 + p), r_x.at[i * 4 + p])
                send(image(i * 4 + p), image(i * 4 + p), r_x.at[i * 4 + p], tp=k1)
            for p in (k1, k3):
                recv(image(i * 4 + p), r_x.at[i * 4 + p])
            if i == 0:
                recv(wr.at[:, pl.ds(mo(k1 * 256, 256), 256)], r_ws.at[0])
                for t in range(5):
                    for s, q in ((0, k2), (1, k3)):
                        recv(wdst(other + t, q), r_wz.at[s, t])
            fwd(i)
            pltpu.make_async_copy(zs.at[pl.ds(i * SET, SET)], z_out.at[pl.ds(i * SET, SET)], s_loc.at[14 + i]).start()
            gsend(z, k, i, tp=k2)
            gsend(z, k, i, dp=zo)
            gsend(z, k, i, tp=k1)
            for j in range(4):
                send(
                    xa.at[pl.ds(((i * 4 + j) * 15 + 1) * 16, ROWS), pl.ds(kc, 256)],
                    xz.at[pl.ds(i * SET + j * ROWS, ROWS)],
                    r_xz.at[i, j],
                    dp=zo,
                )
            put_xt(
                jnp.concatenate(
                    [xa[pl.ds(((i * 4 + j) * 15 + 1) * 16, ROWS), pl.ds(kc, 256)] for j in range(4)], axis=0
                ),
                i,
            )
            if i > 0:
                backward(i - 1)
        dw(0, True, False)
        backward(2)
        for i in range(3):
            grecv(zo, k2, i)
            gsend(zo, k2, i, tp=k1)
            for j in range(4):
                recv(xz.at[pl.ds(i * SET + j * ROWS, ROWS)], r_xz.at[i, j])
            put_xt(xz[pl.ds(i * SET, SET)], 3 + i)
            grecv(zo, k1, i)
            grecv(zo, k3, i)
            if i != 1:
                dw(1 + i // 2, False, i == 2)
        for i in range(3):
            pltpu.make_async_copy(zs.at[pl.ds(i * SET, SET)], z_out.at[pl.ds(i * SET, SET)], s_loc.at[14 + i]).wait()
        for q in range(4):
            qc = pl.ds(q * 256, 256)
            pltpu.make_async_copy(dwa.at[pl.ds(0, 9), :, qc], dw_out.at[:, :, qc], s_loc.at[6 + q]).wait()
            pltpu.make_async_copy(dwa.at[9, :, qc], ds_out.at[:, qc], s_loc.at[10 + q]).wait()
        for c in sends:
            c.wait_send()


def solution(mesh):
    act_spec = P("stage", ("dp", "tp"), None, None, None)
    kernel_spec = P("stage", None, None, "tp", None)
    short_spec = P("stage", "tp", None)
    vec_spec = P("stage", "tp")
    grad_spec = P("stage", "dp", None, None, "tp")

    def device_step(act_in, w_conv, w_short, gamma, beta, gamma_s, grad_z):
        pads = ((0, 0), (0, 0), (0, 2), (0, 0))
        x0 = jnp.pad(act_in[0], pads).reshape(3 * ROWS, 1024)
        dz = jnp.pad(grad_z[0], pads).reshape(4, 3, ROWS, 256).transpose(1, 0, 2, 3).reshape(12 * ROWS, 256)
        vec = jnp.concatenate([gamma, beta, gamma_s, jnp.zeros((5, 256), F32)], axis=0)
        any_spec = pl.BlockSpec(memory_space=pl.ANY)
        dma = pltpu.SemaphoreType.DMA
        z, dx, dw, ds = pl.pallas_call(
            block_kernel,
            out_shape=(
                jax.ShapeDtypeStruct((12 * ROWS, 256), BF),
                jax.ShapeDtypeStruct((3 * ROWS, 1024), BF),
                jax.ShapeDtypeStruct((9, 256, 1024), F32),
                jax.ShapeDtypeStruct((256, 1024), F32),
            ),
            in_specs=[any_spec] * 5,
            out_specs=(any_spec,) * 4,
            scratch_shapes=[
                pltpu.VMEM((12 * HALO + 16, 1024), BF),
                pltpu.VMEM((10, 256, 1024), BF),
                pltpu.VMEM((10, 1024, 256), BF),
                pltpu.VMEM((4, 8, 256), F32),
                pltpu.VMEM((12 * ROWS, 256), BF),
                pltpu.VMEM((2, 4, 12 * ROWS, 256), BF),
                pltpu.VMEM((12 * ROWS, 256), BF),
                pltpu.VMEM((3, 256, 24 * ROWS), BF),
                pltpu.VMEM((8 * HALO + 16, 256), BF),
                pltpu.VMEM((8 * ROWS, 256), BF),
                pltpu.VMEM((4 * HALO + 16, 1024), BF),
                pltpu.VMEM((4 * ROWS, 1024), BF),
                pltpu.VMEM((10, 256, 1024), F32),
                pltpu.VMEM((12 * ROWS, 256), BF),
                pltpu.VMEM((12 * ROWS, 256), BF),
                dma((100,)),
                dma((20,)),
                dma((1,)),
                dma((2, 5)),
                dma((2, 5)),
                dma((3,)),
                dma((12,)),
                dma((3, 4)),
                dma((2, 4, 3)),
                dma((3, 4)),
            ],
            compiler_params=pltpu.CompilerParams(has_side_effects=True, vmem_limit_bytes=67043328),
        )(x0, w_conv[0].reshape(9, 256, 1024), w_short[0], vec, dz)
        on = lax.axis_index("stage") == 1
        z = z.reshape(3, 4, 14, 16, 256).transpose(1, 0, 2, 3, 4).reshape(12, 14, 16, 256)[:, :, :14]
        z = jnp.where(on, z, jnp.zeros_like(z))
        dx = dx.reshape(3, 14, 16, 1024)[:, :, :14]
        dx = jnp.where(on, jnp.zeros_like(dx), dx)
        dw = jnp.where(on, dw, 0.0).reshape(1, 3, 3, 256, 1024)
        ds = jnp.where(on, ds, 0.0)
        return z[None], dx[None], dw, ds[None]

    return jax.shard_map(device_step, mesh=mesh, in_specs=(act_spec, kernel_spec, short_spec, vec_spec, vec_spec, vec_spec, grad_spec), out_specs=(grad_spec, act_spec, kernel_spec, short_spec), check_vma=False)
```

```python
import jax
import jax.numpy as jnp
from jax import lax
from jax.experimental import pallas as pl
from jax.experimental.pallas import tpu as pltpu
from jax.sharding import PartitionSpec as P

BF = jnp.bfloat16
F32 = jnp.float32
MESH = pl.DeviceIdType.MESH
ROWS = 224
HALO = 240
SET = 4 * ROWS
NT = (((1,), (1,)), ((), ()))


def dot(a, b):
    return jnp.dot(a, b, preferred_element_type=F32)


def dot_t(a, b):
    return lax.dot_general(a, b, NT, preferred_element_type=F32)


def mo(v, m):
    return pl.multiple_of(v, m)


def block_kernel(
    act, wc, ws, gam_in, gs_in, bet, dz_in,
    z_out, dx_out, dw_out, ds_out,
    xa, wo, wr, gamv, gsv, dz, ga, xz, xt, gh, gsh, gx, gsx, dwa, zs, dxs, a14,
    s_send, s_loc, r_ws, r_wx, r_wz, r_v, r_x, r_xs, r_xz, r_g, r_dx,
):
    z = lax.axis_index("dp")
    st = lax.axis_index("stage")
    k = lax.axis_index("tp")
    zo = 1 - z
    k1 = k + 1 - 2 * lax.rem(k, 2)
    k2 = lax.rem(k + 2, 4)
    k3 = 3 - k

    def dev(dp=None, stage=None, tp=None):
        return (z if dp is None else dp, st if stage is None else stage, k if tp is None else tp)

    sends = []

    def send(src, dst, rsem, **to):
        c = pltpu.make_async_remote_copy(src, dst, s_send.at[len(sends)], rsem, device_id=dev(**to), device_id_type=MESH)
        c.start()
        sends.append(c)

    def recv(dst, rsem):
        pltpu.make_async_remote_copy(dst, dst, s_send.at[0], rsem, device_id=dev(), device_id_type=MESH).wait_recv()

    def image(n):
        return xa.at[pl.ds(mo((n * 15 + 1) * 16, 16), ROWS)]

    def img_rows(i, j):
        return pl.ds(mo((i * 4 + j) * ROWS, 32), ROWS)

    def zcols(q):
        return pl.ds(mo(q * 256, 256), 256)

    @pl.when(st == 0)
    def _():
        loads = [pltpu.make_async_copy(act.at[i], a14.at[i], s_loc.at[i]) for i in range(3)]
        for c in loads:
            c.start()
        qa = 2 * (k // 2)

        def to_z(i, j):
            for n in range(2):
                src = xa.at[pl.ds(mo(((i * 4 + j) * 15 + 1) * 16, 16), ROWS), zcols(qa + n)]
                send(src, ga.at[0, qa + n, img_rows(i, j)], r_xs.at[i * 4 + j, n], dp=zo)

        def y_image(i, j):
            send(image(i * 4 + j), image(i * 4 + j), r_x.at[i * 4 + j], stage=1)

        for i in range(3):
            loads[i].wait()

            def pad(h, _):
                row = ((i * 4 + k) * 15 + 1 + h) * 16
                xa[pl.ds(mo(row, 16), 16)] = jnp.concatenate([a14[i, h], jnp.zeros((2, 1024), BF)], axis=0)
                return 0

            lax.fori_loop(0, 14, pad, 0)
            if i != 1:
                send(image(i * 4 + k), image(i * 4 + k), r_x.at[i * 4 + k], tp=k2)
            if i < 2:
                y_image(i, k)
        send(image(4 + k), image(4 + k), r_x.at[4 + k], tp=k2)
        for i in range(3):
            to_z(i, k)
        recv(image(k2), r_x.at[k2])
        y_image(0, k2)
        y_image(2, k)
        recv(image(8 + k2), r_x.at[8 + k2])
        y_image(2, k2)
        recv(image(4 + k2), r_x.at[4 + k2])
        for i in range(3):
            to_z(i, k2)
        for i in range(3):
            for j in (k, k2):
                for n in range(2):
                    buf = ga.at[0, qa + n, img_rows(i, j)]
                    recv(buf, r_xs.at[i * 4 + j, n])
                    send(buf, xz.at[img_rows(i, j)], r_xz.at[i, j], stage=1, tp=qa + n)
        zs[...] = jnp.zeros((12, 14, 14, 256), BF)
        fill = pltpu.make_async_copy(zs, z_out, s_loc.at[0])
        fill.start()
        fill.wait()
        for i in range(3):
            for q in range(4):
                recv(dx_out.at[i, :, :, pl.ds(q * 256, 256)], r_dx.at[i, q])
        for c in sends:
            c.wait_send()

    sends.clear()

    @pl.when(st == 1)
    def _():
        kc = mo(k * 256, 256)

        def wsrc(tap, q):
            return wo.at[tap, :, pl.ds(mo(q * 256, 256), 256)]

        def wdst(tap, q):
            return wr.at[tap, pl.ds(mo(q * 256, 256), 256)]

        local = [
            pltpu.make_async_copy(wc, wo.at[pl.ds(0, 9)], s_loc.at[4]),
            pltpu.make_async_copy(ws, wo.at[9], s_loc.at[5]),
            pltpu.make_async_copy(gam_in, gamv.at[k], s_loc.at[2]),
            pltpu.make_async_copy(gs_in, gsv.at[k], s_loc.at[18]),
            pltpu.make_async_copy(dz_in, zs, s_loc.at[3]),
            pltpu.make_async_copy(wc.at[:, :, pl.ds(kc, 256)], wr.at[pl.ds(0, 9), pl.ds(kc, 256)], s_loc.at[0]),
            pltpu.make_async_copy(ws.at[:, pl.ds(kc, 256)], wr.at[9, pl.ds(kc, 256)], s_loc.at[1]),
        ]
        for c in local:
            c.start()
        for c in local[:2]:
            c.wait()
        mine, other = z * 5, zo * 5
        for t in range(5):
            send(wsrc(mine + t, k2), wdst(mine + t, k), r_wx.at[0, t], tp=k2)
            send(wsrc(mine + t, k3), wdst(mine + t, k), r_wx.at[1, t], tp=k3)
        send(
            wo.at[:, :, pl.ds(mo(k1 * 256, 256), 256)], wr.at[:, pl.ds(kc, 256)], r_ws.at[0], tp=k1
        )
        for n, p in enumerate((k1, k2, k3)):
            send(gam_in, gamv.at[k], r_v.at[n, 0], tp=p)
            send(gs_in, gsv.at[k], r_v.at[n, 1], tp=p)

        def zero_rows(n, _):
            xa[pl.ds(mo(n * HALO, 16), 16)] = jnp.zeros((16, 1024), BF)
            return 0

        lax.fori_loop(0, 13, zero_rows, 0)
        for n in range(5):
            gx[pl.ds(n * HALO, 16)] = jnp.zeros((16, 1024), BF)
        for n in range(9):
            gh[pl.ds(n * HALO, 16)] = jnp.zeros((16, 256), BF)

        dxs[...] = jnp.zeros((12, 14, 14, 256), BF)
        for c in local[2:]:
            c.wait()
        fills = [
            pltpu.make_async_copy(dxs.at[pl.ds(0, 3)], dx_out.at[:, :, :, zcols(q)], s_loc.at[6 + q]) for q in range(4)
        ]
        for c in fills:
            c.start()

        def pad_dz(r, _):
            n, h = r // 14, lax.rem(r, 14)
            j, i = n // 3, lax.rem(n, 3)
            row = (i * 4 + j) * ROWS + h * 16
            dz[pl.ds(mo(row, 16), 16)] = jnp.concatenate([zs[n, h], jnp.zeros((2, 256), BF)], axis=0)
            return 0

        lax.fori_loop(0, 168, pad_dz, 0)
        for c in fills:
            c.wait()

        def forward_image(i, j, **to):
            send(image(i * 4 + j), image(i * 4 + j), r_x.at[i * 4 + j], **to)

        def take(i, j):
            recv(image(i * 4 + j), r_x.at[i * 4 + j])

        for t in range(5):
            for s, q in ((0, k2), (1, k3)):
                recv(wdst(mine + t, q), r_wx.at[s, t])
                send(wdst(mine + t, q), wdst(mine + t, q), r_wz.at[s, t], dp=zo)
            if t == 1:
                take(0, k)
                forward_image(0, k, tp=k1)
            if t == 3:
                take(1, k)
                forward_image(1, k, tp=k2)
                forward_image(1, k, tp=k1)

        for n, p in enumerate((k1, k2, k3)):
            recv(gamv.at[p], r_v.at[n, 0])
            recv(gsv.at[p], r_v.at[n, 1])

        def rows_of(b):
            return [mo((b * 2 + n) * HALO, 16) for n in range(2)]

        def fwd(i):
            gam, beta, gsc = gamv[k], bet[...], gsv[k]

            def body(b, _):
                bases = rows_of(i * 2 + b)

                def lhs(t):
                    return jnp.concatenate([xa[pl.ds(mo(s + t * 16, 16), ROWS)] for s in bases], axis=0)

                parts = []
                for j in range(3):
                    acc = dot(lhs(0), wr[j])
                    acc += dot(lhs(1), wr[3 + j])
                    acc += dot(lhs(2), wr[6 + j])
                    parts.append(acc)
                pre = parts[1] + pltpu.roll(parts[0], 1, 0) + pltpu.roll(parts[2], 447, 0)
                u = pre * gam + beta + dot(lhs(1), wr[9]) * gsc
                at = pl.ds(mo(i * SET + b * 448, 64), 448)
                zb = jnp.maximum(u, 0.0).astype(BF)
                for n in range(2):
                    for h in range(14):
                        zs[(b * 2 + n) * 3 + i, h] = zb[(n * 14 + h) * 16:(n * 14 + h) * 16 + 14]
                ga[z, k, at] = jnp.where(u > 0.0, dz[at].astype(F32), 0.0).astype(BF)
                return 0

            lax.fori_loop(0, 2, body, 0)

        def blk(zz, q, i):
            return ga.at[zz, q, pl.ds(i * SET, SET)]

        def gsend(zz, q, i, **to):
            send(blk(zz, q, i), blk(zz, q, i), r_g.at[zz, q, i], **to)

        def grecv(zz, q, i):
            recv(blk(zz, q, i), r_g.at[zz, q, i])

        def put_xt(val, t):
            v = val.astype(F32)
            for j in range(3):
                w = v if j == 1 else pltpu.roll(v, (1 - j) % SET, 0)
                xt[j, :, pl.ds(t * SET, SET)] = w.T.astype(BF)

        def dx(i):
            for q in range(4):
                gam, gsc = gamv[q], gsv[q]

                def scale(n, _):
                    v = ga[z, q, pl.ds(mo(i * SET + n * ROWS, 32), ROWS)].astype(F32)
                    gx[pl.ds(mo(n * HALO + 16, 16), ROWS), pl.ds(q * 256, 256)] = (v * gam).astype(BF)
                    gsx[pl.ds(mo(n * ROWS, 32), ROWS), pl.ds(q * 256, 256)] = (v * gsc).astype(BF)
                    return 0

                lax.fori_loop(0, 4, scale, 0)

            def body(b, _):
                bases = rows_of(b)

                def lhs(t):
                    return jnp.concatenate([gx[pl.ds(mo(s + (2 - t) * 16, 16), ROWS)] for s in bases], axis=0)

                parts = []
                for j in range(3):
                    acc = dot_t(lhs(0), wo[j])
                    acc += dot_t(lhs(1), wo[3 + j])
                    acc += dot_t(lhs(2), wo[6 + j])
                    parts.append(acc)
                tot = parts[1] + pltpu.roll(parts[0], 447, 0) + pltpu.roll(parts[2], 1, 0)
                tot += dot_t(gsx[pl.ds(mo(b * 448, 64), 448)], wo[9])
                db = tot.astype(BF)
                for n in range(2):
                    for h in range(14):
                        dxs[i * 4 + b * 2 + n, h] = db[(n * 14 + h) * 16:(n * 14 + h) * 16 + 14]
                return 0

            lax.fori_loop(0, 2, body, 0)
            for j in range(4):
                send(
                    dxs.at[i * 4 + j],
                    dx_out.at[i, :, :, pl.ds(kc, 256)],
                    r_dx.at[i, k],
                    stage=0, tp=j,
                )

        def quarter(n):
            b = lax.rem(k + 2 * (n // 2), 4)
            return b + lax.rem(n, 2) * (1 - 2 * lax.rem(b, 2))

        def dw(u, first, last, lo=0, hi=4):
            def per_q(nq, _):
                q = quarter(nq)
                gam, gsc = gamv[q], gsv[q]
                qc = pl.ds(mo(q * 256, 256), 256)

                def scale(n, _):
                    t = u * 8 + n
                    zz = jnp.where(t < 12, z, zo)
                    v = ga[zz, q, pl.ds(mo(lax.rem(t, 12) * ROWS, 32), ROWS)].astype(F32)
                    gh[pl.ds(mo(n * HALO + 16, 16), ROWS)] = (v * gam).astype(BF)
                    gsh[pl.ds(mo(n * ROWS, 32), ROWS)] = (v * gsc).astype(BF)
                    return 0

                lax.fori_loop(0, 8, scale, 0)
                lanes = pl.ds(u * 1792, 1792)
                for i in range(3):
                    rhs = jnp.concatenate([gh[pl.ds(n * HALO + (2 - i) * 16, ROWS)] for n in range(8)], axis=0)
                    for j in range(3):
                        d = dot(xt[j, :, lanes], rhs)
                        if first:
                            dwa[3 * i + j, :, qc] = d
                        else:
                            dwa[3 * i + j, :, qc] += d
                d = dot(xt[1, :, lanes], gsh[...])
                if first:
                    dwa[9, :, qc] = d
                else:
                    dwa[9, :, qc] += d
                if last:
                    pltpu.make_async_copy(dwa.at[pl.ds(0, 9), :, qc], dw_out.at[:, :, qc], s_loc.at[6 + nq]).start()
                    pltpu.make_async_copy(dwa.at[9, :, qc], ds_out.at[:, qc], s_loc.at[10 + nq]).start()
                return 0

            lax.fori_loop(lo, hi, per_q, 0)

        def collect(i):
            for j in (k1, k3):
                take(i, j)

        def forward(i):
            fwd(i)
            gsend(z, k, i, tp=k2)
            gsend(z, k, i, dp=zo)
            gsend(z, k, i, tp=k1)
            put_xt(
                jnp.concatenate(
                    [xa[pl.ds(((i * 4 + j) * 15 + 1) * 16, ROWS), pl.ds(kc, 256)] for j in range(4)], axis=0
                ),
                i,
            )

        def relay_x(i):
            grecv(z, k2, i)
            gsend(z, k2, i, tp=k1)
            if i == 1:
                gsend(z, k2, i, dp=zo)

        def relay_z(i):
            grecv(zo, k, i)
            if i != 1:
                gsend(zo, k, i, tp=k2)
            gsend(zo, k, i, tp=k1)

        def backward(i):
            grecv(z, k3, i)
            dx(i)

        take(0, k2)
        forward_image(0, k2, tp=k1)
        collect(0)
        recv(wr.at[:, pl.ds(mo(k1 * 256, 256), 256)], r_ws.at[0])
        for t in range(5):
            for s, q in ((0, k2), (1, k3)):
                recv(wdst(other + t, q), r_wz.at[s, t])
        forward(0)
        take(1, k2)
        forward_image(1, k2, tp=k1)
        take(2, k)
        forward_image(2, k, tp=k1)
        collect(1)
        forward(1)
        grecv(z, k1, 0)
        grecv(z, k1, 1)
        relay_x(0)
        relay_z(0)
        dw(0, True, False, 0, 2)
        take(2, k2)
        forward_image(2, k2, tp=k1)
        collect(2)
        forward(2)
        relay_x(1)
        relay_z(1)
        backward(0)
        backward(1)
        zcopy = pltpu.make_async_copy(zs, z_out, s_loc.at[14])
        zcopy.start()
        relay_x(2)
        relay_z(2)
        dw(0, True, False, 2, 4)
        grecv(z, k1, 2)
        backward(2)
        for i in range(3):
            grecv(zo, k2, i)
            gsend(zo, k2, i, tp=k1)
            for j in range(4):
                recv(xz.at[pl.ds(i * SET + j * ROWS, ROWS)], r_xz.at[i, j])
            put_xt(xz[pl.ds(i * SET, SET)], 3 + i)
            grecv(zo, k1, i)
            grecv(zo, k3, i)
            if i != 1:
                dw(1 + i // 2, False, i == 2)
        zcopy.wait()
        for n in range(4):
            qc = zcols(quarter(n))
            pltpu.make_async_copy(dwa.at[pl.ds(0, 9), :, qc], dw_out.at[:, :, qc], s_loc.at[6 + n]).wait()
            pltpu.make_async_copy(dwa.at[9, :, qc], ds_out.at[:, qc], s_loc.at[10 + n]).wait()
        for c in sends:
            c.wait_send()


def solution(mesh):
    act_spec = P("stage", ("dp", "tp"), None, None, None)
    kernel_spec = P("stage", None, None, "tp", None)
    short_spec = P("stage", "tp", None)
    vec_spec = P("stage", "tp")
    grad_spec = P("stage", "dp", None, None, "tp")

    def device_step(act_in, w_conv, w_short, gamma, beta, gamma_s, grad_z):
        any_spec = pl.BlockSpec(memory_space=pl.ANY)
        dma = pltpu.SemaphoreType.DMA
        z, dx, dw, ds = pl.pallas_call(
            block_kernel,
            out_shape=(
                jax.ShapeDtypeStruct((12, 14, 14, 256), BF),
                jax.ShapeDtypeStruct((3, 14, 14, 1024), BF),
                jax.ShapeDtypeStruct((9, 256, 1024), F32),
                jax.ShapeDtypeStruct((256, 1024), F32),
            ),
            in_specs=[any_spec] * 5 + [pl.BlockSpec(memory_space=pltpu.VMEM), any_spec],
            out_specs=(any_spec,) * 4,
            scratch_shapes=[
                pltpu.VMEM((12 * HALO + 16, 1024), BF),
                pltpu.VMEM((10, 256, 1024), BF),
                pltpu.VMEM((10, 1024, 256), BF),
                pltpu.VMEM((4, 1, 256), F32),
                pltpu.VMEM((4, 1, 256), F32),
                pltpu.VMEM((12 * ROWS, 256), BF),
                pltpu.VMEM((2, 4, 12 * ROWS, 256), BF),
                pltpu.VMEM((12 * ROWS, 256), BF),
                pltpu.VMEM((3, 256, 24 * ROWS), BF),
                pltpu.VMEM((8 * HALO + 16, 256), BF),
                pltpu.VMEM((8 * ROWS, 256), BF),
                pltpu.VMEM((4 * HALO + 16, 1024), BF),
                pltpu.VMEM((4 * ROWS, 1024), BF),
                pltpu.VMEM((10, 256, 1024), F32),
                pltpu.VMEM((12, 14, 14, 256), BF),
                pltpu.VMEM((12, 14, 14, 256), BF),
                pltpu.VMEM((3, 14, 14, 1024), BF),
                dma((100,)),
                dma((20,)),
                dma((1,)),
                dma((2, 5)),
                dma((2, 5)),
                dma((3, 2)),
                dma((12,)),
                dma((12, 2)),
                dma((3, 4)),
                dma((2, 4, 3)),
                dma((3, 4)),
            ],
            compiler_params=pltpu.CompilerParams(has_side_effects=True, vmem_limit_bytes=67043328),
        )(act_in[0], w_conv[0].reshape(9, 256, 1024), w_short[0], gamma, gamma_s, beta, grad_z[0])
        on = lax.axis_index("stage") == 1
        dw = jnp.where(on, dw, 0.0).reshape(1, 3, 3, 256, 1024)
        ds = jnp.where(on, ds, 0.0)
        return z[None], dx[None], dw, ds[None]

    return jax.shard_map(device_step, mesh=mesh, in_specs=(act_spec, kernel_spec, short_spec, vec_spec, vec_spec, vec_spec, grad_spec), out_specs=(grad_spec, act_spec, kernel_spec, short_spec), check_vma=False)
```

```python
import jax
import jax.numpy as jnp
from jax import lax
from jax.experimental import pallas as pl
from jax.experimental.pallas import tpu as pltpu
from jax.sharding import PartitionSpec as P

BF = jnp.bfloat16
F32 = jnp.float32
MESH = pl.DeviceIdType.MESH
PARTS = 4
LANES = 256
CHANNELS = 1024
WIDE = 16
SIDE = 14
TAPS = 9
IMAGES = 12
PAIR = 448
ROWS = 224
HALO = 240
SET = 4 * ROWS
UNIT = 8 * ROWS
NT = (((1,), (1,)), ((), ()))


def dot(a, b):
    return jnp.dot(a, b, preferred_element_type=F32)


def dot_t(a, b):
    return lax.dot_general(a, b, NT, preferred_element_type=F32)


def mo(v, m):
    return pl.multiple_of(v, m)


def zcols(q):
    return pl.ds(mo(q * LANES, LANES), LANES)


def scale_block(value, gam, gsc, gh, gsh):
    for n in range(8):
        v = value(n).astype(F32)
        gh[n * HALO + WIDE:n * HALO + HALO] = (v * gam).astype(BF)
        gsh[n * ROWS:n * ROWS + ROWS] = (v * gsc).astype(BF)


def weight_dots(xt, lanes, gh, gsh, put):
    for i in range(3):
        rhs = jnp.concatenate([gh[n * HALO + (2 - i) * WIDE:n * HALO + (2 - i) * WIDE + ROWS] for n in range(8)], axis=0)
        for j in range(3):
            put(3 * i + j, dot(xt[j, :, lanes], rhs))
    put(TAPS, dot(xt[1, :, lanes], gsh[...]))


def block_kernel(
    act, wc, ws, gam_in, gs_in, bet, dz_in,
    z_out, dx_out, acc_out, xt_out, g_out, gam_out, gs_out,
    xa, wo, wr, gamv, gsv, dz, ga, xz, xt, gh0, gsh0, gh1, gsh1, gx, gsx, dwa, zs, dxs,
    s_send, s_loc, s_tail, r_ws, r_wx, r_wz, r_v, r_x, r_xs, r_xz, r_g, r_dx, r_rel, r_h,
):
    z = lax.axis_index("dp")
    st = lax.axis_index("stage")
    k = lax.axis_index("tp")
    zo = 1 - z
    k1 = k + 1 - 2 * lax.rem(k, 2)
    k2 = lax.rem(k + 2, PARTS)
    k3 = 3 - k
    kx = k // 2
    qa = 2 * kx
    kc = mo(k * LANES, LANES)

    def dev(dp=None, stage=None, tp=None):
        return (z if dp is None else dp, st if stage is None else stage, k if tp is None else tp)

    sends = []

    def remote(src, dst, ssem, rsem, **to):
        return pltpu.make_async_remote_copy(src, dst, ssem, rsem, device_id=dev(**to), device_id_type=MESH)

    def send(src, dst, rsem, **to):
        c = remote(src, dst, s_send.at[len(sends)], rsem, **to)
        c.start()
        sends.append(c)

    def recv(dst, rsem):
        remote(dst, dst, s_send.at[0], rsem).wait_recv()

    def image(i, j):
        return xa.at[pl.ds(mo(((i * PARTS + j) * 15 + 1) * WIDE, WIDE), ROWS)]

    def img_rows(i, j):
        return pl.ds(mo((i * PARTS + j) * ROWS, 32), ROWS)

    barrier = pltpu.get_barrier_semaphore()

    def greet(peers):
        for p in peers:
            pl.semaphore_signal(barrier, inc=1, device_id=dev(**p), device_id_type=MESH)
        pl.semaphore_wait(barrier, len(peers))

    @pl.when(st == 0)
    def _():
        loads = [
            pltpu.make_async_copy(act.at[i, :, :, zcols(q)], zs.at[i * PARTS + q], s_loc.at[i * PARTS + q])
            for i in range(3) for q in range(PARTS)
        ]
        for c in loads:
            c.start()
        greet([dict(tp=k2), dict(dp=zo), dict(stage=1, tp=qa), dict(stage=1, tp=qa + 1)])

        def to_z(i, j):
            for n in range(2):
                src = xa.at[pl.ds(mo(((i * PARTS + j) * 15 + 1) * WIDE, WIDE), ROWS), zcols(qa + n)]
                send(src, ga.at[0, qa + n, img_rows(i, j)], r_xs.at[i * PARTS + j, n], dp=zo)

        def y_image(i, j):
            send(image(i, j), image(i, j), r_x.at[i * PARTS + j], stage=1)

        def x_image(i):
            send(image(i, k), image(i, k), r_x.at[i * PARTS + k], tp=k2)

        for i in range(3):
            for c in loads[PARTS * i:PARTS * i + PARTS]:
                c.wait()

            def pad(h, _):
                rows = pl.ds(mo(((i * PARTS + k) * 15 + 1 + h) * WIDE, WIDE), WIDE)
                for q in range(PARTS):
                    xa[rows, q * LANES:q * LANES + LANES] = jnp.concatenate([zs[i * PARTS + q, h], jnp.zeros((2, LANES), BF)], axis=0)
                return 0

            lax.fori_loop(0, SIDE, pad, 0)
            if i == 0:
                x_image(0)
                y_image(0, k)
            if i == 1:
                y_image(1, k)
        x_image(2)
        x_image(1)
        for i in range(3):
            to_z(i, k)
        recv(image(0, k2), r_x.at[k2])
        y_image(0, k2)
        y_image(2, k)
        recv(image(2, k2), r_x.at[8 + k2])
        y_image(2, k2)
        recv(image(1, k2), r_x.at[PARTS + k2])
        for i in range(3):
            to_z(i, k2)
        for i in range(3):
            for j in (k, k2):
                for n in range(2):
                    buf = ga.at[0, qa + n, img_rows(i, j)]
                    recv(buf, r_xs.at[i * PARTS + j, n])
                    send(buf, xz.at[img_rows(i, j)], r_xz.at[i, j], stage=1, tp=qa + n)
        zs[...] = jnp.zeros((IMAGES, SIDE, SIDE, LANES), BF)
        fill = pltpu.make_async_copy(zs, z_out, s_loc.at[0])
        fill.start()
        fill.wait()
        for i in range(3):
            for n in range(2):
                q = qa + n
                recv(dxs.at[i * PARTS + q], r_rel.at[i, q])
                send(dxs.at[i * PARTS + q], dx_out.at[i, :, :, zcols(q)], r_dx.at[i, q], tp=k2)
        for i in range(3):
            for q in range(PARTS):
                recv(dx_out.at[i, :, :, zcols(q)], r_dx.at[i, q])
        for c in sends:
            c.wait_send()

    sends.clear()

    @pl.when(st == 1)
    def _():
        local = [
            pltpu.make_async_copy(dz_in, zs, s_loc.at[0]),
            pltpu.make_async_copy(gam_in, gamv.at[k], s_loc.at[1]),
            pltpu.make_async_copy(gs_in, gsv.at[k], s_loc.at[2]),
            pltpu.make_async_copy(wc.at[:, :, pl.ds(kc, LANES)], wr.at[pl.ds(0, TAPS), pl.ds(kc, LANES)], s_loc.at[3]),
            pltpu.make_async_copy(ws.at[:, pl.ds(kc, LANES)], wr.at[TAPS, pl.ds(kc, LANES)], s_loc.at[PARTS]),
            pltpu.make_async_copy(wc, wo.at[pl.ds(0, TAPS)], s_loc.at[5]),
            pltpu.make_async_copy(ws, wo.at[TAPS], s_loc.at[6]),
        ]
        for c in local:
            c.start()

        def zero_rows(n, _):
            xa[pl.ds(mo(n * HALO, WIDE), WIDE)] = jnp.zeros((WIDE, CHANNELS), BF)
            return 0

        lax.fori_loop(0, 13, zero_rows, 0)
        greet([dict(tp=k1), dict(tp=k2), dict(tp=k3), dict(dp=zo), dict(stage=0, tp=qa), dict(stage=0, tp=qa + 1)])

        def wdst(tap, q):
            return wr.at[tap, zcols(q)]

        mine, other = z * 5, zo * 5

        def wsend(t, q, n):
            ssem, rsem = s_send.at[len(sends)], r_wx.at[n, t]
            if t < PARTS:
                send(wc.at[mine + t, :, zcols(q)], wdst(mine + t, k), rsem, tp=q)
                return

            @pl.when(z == 0)
            def _():
                remote(wc.at[PARTS, :, zcols(q)], wdst(PARTS, k), ssem, rsem, tp=q).start()

            @pl.when(z == 1)
            def _():
                remote(ws.at[:, zcols(q)], wdst(TAPS, k), ssem, rsem, tp=q).start()

            sends.append(remote(ws.at[:, zcols(q)], wdst(TAPS, k), ssem, rsem, tp=q))

        for n, p in enumerate((k1, k2, k3)):
            send(gam_in, gamv.at[k], r_v.at[n, 0], tp=p)
            send(gs_in, gsv.at[k], r_v.at[n, 1], tp=p)
        for t in range(5):
            wsend(t, k2, 0)
            wsend(t, k3, 1)
        send(wc.at[:, :, zcols(k1)], wr.at[pl.ds(0, TAPS), pl.ds(kc, LANES)], r_ws.at[0], tp=k1)
        send(ws.at[:, zcols(k1)], wr.at[TAPS, pl.ds(kc, LANES)], r_ws.at[1], tp=k1)
        def set_up():
            for n in range(5):
                gx[pl.ds(n * HALO, WIDE)] = jnp.zeros((WIDE, CHANNELS), BF)
            for n in range(TAPS):
                gh0[pl.ds(n * HALO, WIDE)] = jnp.zeros((WIDE, LANES), BF)
                gh1[pl.ds(n * HALO, WIDE)] = jnp.zeros((WIDE, LANES), BF)
            dxs[0:3] = jnp.zeros((3, SIDE, SIDE, LANES), BF)
            for c in local:
                c.wait()
            for c in fills:
                c.start()

        fills = [
            pltpu.make_async_copy(dxs.at[pl.ds(0, 3)], dx_out.at[:, :, :, zcols(q)], s_loc.at[10 + q]) for q in range(PARTS)
        ]

        def pad_dz(n, _):
            row = (lax.rem(n, 3) * PARTS + n // 3) * ROWS
            for h in range(SIDE):
                dz[pl.ds(mo(row + h * WIDE, WIDE), WIDE)] = jnp.concatenate([zs[n, h], jnp.zeros((2, LANES), BF)], axis=0)
            return 0

        def take(i, j):
            recv(image(i, j), r_x.at[i * PARTS + j])

        def pass_on(i, j, tp):
            send(image(i, j), image(i, j), r_x.at[i * PARTS + j], tp=tp)

        def fwd(i, b, mode):
            gam, beta, gsc = gamv[k], bet[...], gsv[k]
            bases = [mo((i * PARTS + b * 2 + n) * HALO, WIDE) for n in range(2)]
            ch = {
                "all": pl.ds(0, CHANNELS),
                "own": pl.ds(mo(kx * 512, 512), 512),
                "rest": pl.ds(mo((1 - kx) * 512, 512), 512),
            }[mode]

            def lhs(t):
                return jnp.concatenate([xa[pl.ds(mo(s + t * WIDE, WIDE), ROWS), ch] for s in bases], axis=0)

            parts = []
            for j in range(3):
                acc = dot(lhs(0), wr[j, ch])
                acc += dot(lhs(1), wr[3 + j, ch])
                acc += dot(lhs(2), wr[6 + j, ch])
                parts.append(acc)
            pre = parts[1] + pltpu.roll(parts[0], 1, 0) + pltpu.roll(parts[2], 447, 0)
            u = pre * gam + dot(lhs(1), wr[TAPS, ch]) * gsc
            if mode == "own":
                for n in range(2):
                    dwa[b * 2 + n, 0:ROWS, i * LANES:i * LANES + LANES] = u[n * ROWS:n * ROWS + ROWS]
                return
            if mode == "rest":
                u += jnp.concatenate([dwa[b * 2 + n, 0:ROWS, i * LANES:i * LANES + LANES] for n in range(2)], axis=0)
            u += beta
            at = pl.ds(mo(i * SET + b * PAIR, 64), PAIR)
            zb = jnp.maximum(u, 0.0).astype(BF)
            for n in range(2):
                for h in range(SIDE):
                    zs[(b * 2 + n) * 3 + i, h] = zb[(n * SIDE + h) * WIDE:(n * SIDE + h) * WIDE + SIDE]
            ga[z, k, at] = jnp.where(u > 0.0, dz[at].astype(F32), 0.0).astype(BF)

        def fwd_set(i, mode):
            def body(b, _):
                fwd(i, b, mode)
                return 0

            lax.fori_loop(0, 2, body, 0)

        def blk(zz, q, i):
            return ga.at[zz, q, pl.ds(mo(i * SET, 128), SET)]

        def gsend(zz, q, i, **to):
            send(blk(zz, q, i), blk(zz, q, i), r_g.at[zz, q, i], **to)

        def grecv(zz, q, i):
            recv(blk(zz, q, i), r_g.at[zz, q, i])

        def put_xt(val, t):
            v = val.astype(F32)
            for j in range(3):
                w = v if j == 1 else pltpu.roll(v, (1 - j) % SET, 0)
                xt[j, :, pl.ds(t * SET, SET)] = w.T.astype(BF)

        def dx(i, n0):
            for q in range(PARTS):
                gam, gsc = gamv[q], gsv[q]

                def scale(n, _):
                    v = ga[z, q, pl.ds(mo(i * SET + n * ROWS, 32), ROWS)].astype(F32)
                    gx[pl.ds(mo(n * HALO + WIDE, WIDE), ROWS), pl.ds(q * LANES, LANES)] = (v * gam).astype(BF)
                    gsx[pl.ds(mo(n * ROWS, 32), ROWS), pl.ds(q * LANES, LANES)] = (v * gsc).astype(BF)
                    return 0

                lax.fori_loop(0, PARTS, scale, 0)

            def body(b):
                bases = [mo((b * 2 + n) * HALO, WIDE) for n in range(2)]

                def lhs(t):
                    return jnp.concatenate([gx[pl.ds(mo(s + (2 - t) * WIDE, WIDE), ROWS)] for s in bases], axis=0)

                parts = []
                for j in range(3):
                    acc = dot_t(lhs(0), wo[j])
                    acc += dot_t(lhs(1), wo[3 + j])
                    acc += dot_t(lhs(2), wo[6 + j])
                    parts.append(acc)
                tot = parts[1] + pltpu.roll(parts[0], 447, 0) + pltpu.roll(parts[2], 1, 0)
                tot += dot_t(gsx[pl.ds(mo(b * PAIR, 64), PAIR)], wo[TAPS])
                db = tot.astype(BF)
                for n in range(2):
                    for h in range(SIDE):
                        dxs[i * PARTS + b * 2 + n, h] = db[(n * SIDE + h) * WIDE:(n * SIDE + h) * WIDE + SIDE]

            def step(m, _):
                body(jnp.where(m == 0, 1 - kx, kx))

                @pl.when(m == 0)
                def _():
                    for j, via, ssem in out[0]:
                        remote(dxs.at[i * PARTS + j], dxs.at[i * PARTS + k], ssem, r_rel.at[i, k], stage=0, tp=via).start()

                @pl.when(m == 1)
                def _():
                    for j, via, ssem in out[1]:
                        remote(
                            dxs.at[i * PARTS + j], dx_out.at[i, :, :, pl.ds(kc, LANES)], ssem, r_dx.at[i, k], stage=0, tp=via
                        ).start()

                return 0

            out = (
                ((k2, k, s_send.at[n0]), (k3, k1, s_send.at[n0 + 1])),
                ((k, k, s_send.at[n0 + 2]), (k1, k1, s_send.at[n0 + 3])),
            )
            lax.fori_loop(0, 2, step, 0)

        def dx_sends(count):
            n0 = len(sends)
            for n in range(PARTS * count):
                sends.append(remote(dxs.at[0], dxs.at[0], s_send.at[n0 + n], r_rel.at[0, 0]))
            return n0

        def quarter(n):
            b = lax.rem(k + 2 * (n // 2), PARTS)
            return b + lax.rem(n, 2) * (1 - 2 * lax.rem(b, 2))

        def dw(u, first, lo, hi, between=None):
            bufs = ((gh0, gsh0), (gh1, gsh1))

            def scale(n, m):
                q = quarter(n)

                def value(r):
                    t = u * 8 + r
                    zz = z if t < IMAGES else zo
                    return ga[zz, q, pl.ds((t % IMAGES) * ROWS, ROWS)]

                scale_block(value, gamv[q], gsv[q], *bufs[m])

            def pair(half, _):
                if between is not None:
                    pl.when(half == 1)(between)
                for m in range(2):
                    n = 2 * half + m
                    cols = zcols(quarter(n))

                    def put(tap, d):
                        if first:
                            dwa[tap, :, cols] = d
                        else:
                            dwa[tap, :, cols] += d

                    if m == 0:
                        scale(n + 1, 1)
                    elif hi - lo > 1:
                        scale(jnp.minimum(n + 1, 3), 0)
                    weight_dots(xt, pl.ds(u * UNIT, UNIT), *bufs[m], put)
                    if not first:
                        pltpu.make_async_copy(dwa.at[:, :, cols], acc_out.at[:, :, cols], s_loc.at[10 + n]).start()
                return 0

            scale(2 * lo, 0)
            lax.fori_loop(lo, hi, pair, 0)

        def collect(i):
            take(i, k1)
            take(i, k3)

        def own_xt(i):
            put_xt(
                jnp.concatenate(
                    [xa[pl.ds(((i * PARTS + j) * 15 + 1) * WIDE, ROWS), pl.ds(kc, LANES)] for j in range(PARTS)], axis=0
                ),
                i,
            )

        def spread(i):
            gsend(z, k, i, tp=k2)
            gsend(z, k, i, dp=zo)
            gsend(z, k, i, tp=k1)
            own_xt(i)

        def relay(zz, q, i, ssem):
            grecv(zz, q, i)
            if ssem is None:
                gsend(zz, q, i, tp=k1)
            else:
                remote(blk(zz, q, i), blk(zz, q, i), ssem, r_g.at[zz, q, i], tp=k1).start()

        def relay_x(i, ssem=None):
            relay(z, k2, i, ssem)

        def relay_z(i, ssem=None):
            relay(zo, k, i, ssem)

        def half(zz, q, i, h):
            return ga.at[zz, q, pl.ds(i * SET + h * PAIR, PAIR)]

        def diagonal(i):
            send(half(zo, k, i, 0), half(zo, k, i, 0), r_h.at[i, 0], tp=k2)
            send(half(z, k2, i, 1), half(z, k2, i, 1), r_h.at[i, 1], dp=zo)

        def arrive(i, ssem):
            recv(half(zo, k2, i, 0), r_h.at[i, 0])
            recv(half(zo, k2, i, 1), r_h.at[i, 1])
            remote(blk(zo, k2, i), blk(zo, k2, i), ssem, r_g.at[zo, k2, i], tp=k1).start()
            for j in range(PARTS):
                recv(xz.at[pl.ds(i * SET + j * ROWS, ROWS)], r_xz.at[i, j])
            put_xt(xz[pl.ds(i * SET, SET)], 3 + i)

        def results(i, which):
            at = pl.ds((i - 1) * SET, SET)
            pairs = [(blk(zo, q, i), g_out.at[q, at]) for q in ((k1, k3) if which else (k, k2))]
            if which == 0:
                pairs.append((xt.at[:, :, pl.ds((3 + i) * SET, SET)], xt_out.at[:, :, at]))
            return [pltpu.make_async_copy(a, b, s_tail.at[i - 1, which, n]) for n, (a, b) in enumerate(pairs)]

        def leave(i, which):
            for c in results(i, which):
                c.start()

        for t in range(5):
            for s, q in ((0, k2), (1, k3)):
                recv(wdst(mine + t, q), r_wx.at[s, t])
                send(wdst(mine + t, q), wdst(mine + t, q), r_wz.at[s, t], dp=zo)
            if t == 0:
                set_up()
                for n, p in enumerate((k1, k2, k3)):
                    recv(gamv.at[p], r_v.at[n, 0])
                    recv(gsv.at[p], r_v.at[n, 1])
                recv(wr.at[pl.ds(0, TAPS), zcols(k1)], r_ws.at[0])
                recv(wr.at[TAPS, zcols(k1)], r_ws.at[1])
            if t == 1:
                lax.fori_loop(0, IMAGES, pad_dz, 0)
                take(0, k)
                pass_on(0, k, k1)
            if t == 2:
                for c in fills:
                    c.wait()
                take(0, k1)
                fwd(0, kx, "own")
            if t == 3:
                take(1, k)
                pass_on(1, k, k2)
                pass_on(1, k, k1)
        take(1, k1)
        fwd(1, kx, "own")
        take(0, k2)
        pass_on(0, k2, k1)
        take(0, k3)
        fwd(0, 1 - kx, "own")
        for t in range(5):
            for s, q in ((0, k2), (1, k3)):
                recv(wdst(other + t, q), r_wz.at[s, t])
        fwd_set(0, "rest")
        spread(0)
        fwd(1, kx, "rest")
        take(1, k2)
        pass_on(1, k2, k1)
        take(2, k)
        pass_on(2, k, k1)
        take(1, k3)
        fwd(1, 1 - kx, "all")
        spread(1)
        grecv(z, k1, 0)
        grecv(z, k1, 1)
        dw(0, True, 0, 1)
        relay_z(0)
        relay_x(0)
        diagonal(0)
        n01 = dx_sends(2)

        def dx_of(i, n0):
            grecv(z, k3, i)
            dx(i, n0)

        take(2, k2)
        pass_on(2, k2, k1)

        def first_two(i, _):
            dx_of(i, n01 + PARTS * i)

            @pl.when(i == 0)
            def _():
                collect(2)
                relay_x(1, s_send.at[nsp + 3])
                relay_z(1, s_send.at[nsp + PARTS])
                fwd_set(2, "all")
                for n, (q, to) in enumerate(own_to):
                    remote(blk(z, k, 2), blk(z, k, 2), s_send.at[nsp + n], r_g.at[z, k, 2], **to).start()
                for n, (zz, q, h, to) in enumerate(across):
                    part = half(zz, q, 1, h)
                    remote(part, part, s_send.at[nsp + 5 + n], r_h.at[1, h], **to).start()
                own_xt(2)

            return 0

        nsp = len(sends)
        own_to = ((k2, dict(tp=k2)), (k, dict(dp=zo)), (k1, dict(tp=k1)))
        across = ((zo, k, 0, dict(tp=k2)), (z, k2, 1, dict(dp=zo)))
        for n in range(5):
            sends.append(remote(blk(z, k, 2), blk(z, k, 2), s_send.at[nsp + n], r_g.at[z, k, 2]))
        for n in range(2):
            sends.append(remote(half(z, k, 2, n), half(z, k, 2, n), s_send.at[nsp + 5 + n], r_h.at[1, n]))
        lax.fori_loop(0, 2, first_two, 0)
        zcopy = pltpu.make_async_copy(zs, z_out, s_loc.at[8])
        zcopy.start()
        dw(0, True, 1, 2)
        relay_x(2)
        relay_z(2)
        diagonal(2)
        nar = len(sends)
        for i in range(3):
            sends.append(remote(blk(zo, k2, i), blk(zo, k2, i), s_send.at[nar + i], r_g.at[zo, k2, i]))
        arrive(0, s_send.at[nar])
        grecv(z, k1, 2)
        dx_of(2, dx_sends(1))
        copies = [
            pltpu.make_async_copy(gamv, gam_out, s_loc.at[6]),
            pltpu.make_async_copy(gsv, gs_out, s_loc.at[7]),
        ]
        for c in copies:
            c.start()
        arrive(1, s_send.at[nar + 1])
        leave(1, 0)
        grecv(zo, k1, 0)
        grecv(zo, k3, 0)

        def last_set():
            arrive(2, s_send.at[nar + 2])
            leave(2, 0)
            grecv(zo, k1, 1)
            grecv(zo, k3, 1)
            leave(1, 1)

        dw(1, False, 0, 2, last_set)
        grecv(zo, k1, 2)
        grecv(zo, k3, 2)
        leave(2, 1)
        tail = [c for i in (1, 2) for which in range(2) for c in results(i, which)]
        for c in tail + copies + [zcopy]:
            c.wait()
        for n in range(PARTS):
            cols = zcols(quarter(n))
            pltpu.make_async_copy(dwa.at[:, :, cols], acc_out.at[:, :, cols], s_loc.at[10 + n]).wait()
        for c in sends:
            c.wait_send()


def last_kernel(
    z_in, dx_in, acc, xt_in, g_in, gamv, gsv,
    z_out, dx_out, dw_out, ds_out,
    xt, g, gh0, gsh0, gh1, gsh1, dwa, zb, dxb,
    sem,
):
    st = lax.axis_index("stage")
    bounce = [
        (pltpu.make_async_copy(z_in, zb, sem.at[0]), pltpu.make_async_copy(zb, z_out, sem.at[1])),
        (pltpu.make_async_copy(dx_in, dxb, sem.at[2]), pltpu.make_async_copy(dxb, dx_out, sem.at[3])),
    ]

    def outs(q):
        cols = zcols(q)
        return (
            pltpu.make_async_copy(dwa.at[q, pl.ds(0, TAPS)], dw_out.at[:, :, cols], sem.at[PARTS + 2 * q]),
            pltpu.make_async_copy(dwa.at[q, TAPS], ds_out.at[:, cols], sem.at[5 + 2 * q]),
        )

    @pl.when(st == 0)
    def _():
        for c, _n in bounce:
            c.start()

        def zero(tap, _):
            for q in range(PARTS):
                dwa[q, tap] = jnp.zeros((LANES, LANES), F32)
            return 0

        lax.fori_loop(0, 10, zero, 0)
        for q in range(PARTS):
            for c in outs(q):
                c.start()
        for c, n in bounce:
            c.wait()
            n.start()
        for _c, n in bounce:
            n.wait()
        for q in range(PARTS):
            for c in outs(q):
                c.wait()

    @pl.when(st == 1)
    def _():
        loads = [pltpu.make_async_copy(g_in.at[0], g.at[0], sem.at[IMAGES])]
        loads += [pltpu.make_async_copy(xt_in.at[j], xt.at[j], sem.at[WIDE + j]) for j in range(3)]
        accs = [pltpu.make_async_copy(acc.at[:, :, zcols(q)], dwa.at[q], sem.at[20 + q]) for q in range(PARTS)]
        more = [pltpu.make_async_copy(g_in.at[q], g.at[q], sem.at[IMAGES + q]) for q in range(1, PARTS)]
        for c in [*loads, accs[0], more[0], accs[1], *more[1:], *accs[2:]]:
            c.start()
        for c, _n in bounce:
            c.start()
        for n in range(TAPS):
            gh0[pl.ds(n * HALO, WIDE)] = jnp.zeros((WIDE, LANES), BF)
            gh1[pl.ds(n * HALO, WIDE)] = jnp.zeros((WIDE, LANES), BF)
        bufs = ((gh0, gsh0), (gh1, gsh1))

        def scale(q, m):
            def value(n):
                return g[q, pl.ds(n * ROWS, ROWS)]

            scale_block(value, gamv[q], gsv[q], *bufs[m])

        loads[0].wait()
        scale(0, 0)
        for c in loads[1:]:
            c.wait()

        def pair(half, _):
            @pl.when(half == 1)
            def _():
                for c, n in bounce:
                    c.wait()
                    n.start()

            for m in range(2):
                q = 2 * half + m
                pltpu.make_async_copy(acc.at[:, :, zcols(q)], dwa.at[q], sem.at[20 + q]).wait()
                after = jnp.minimum(q + 1, 3)

                @pl.when(q < 3)
                def _():
                    pltpu.make_async_copy(g_in.at[after], g.at[after], sem.at[IMAGES + after]).wait()

                scale(after, 1 - m)

                def put(tap, d):
                    dwa[q, tap] += d

                weight_dots(xt, pl.ds(0, UNIT), *bufs[m], put)
                for c in outs(q):
                    c.start()
            return 0

        lax.fori_loop(0, 2, pair, 0)
        for _c, n in bounce:
            n.wait()
        for q in range(PARTS):
            for c in outs(q):
                c.wait()


def solution(mesh):
    act_spec = P("stage", ("dp", "tp"), None, None, None)
    kernel_spec = P("stage", None, None, "tp", None)
    short_spec = P("stage", "tp", None)
    vec_spec = P("stage", "tp")
    grad_spec = P("stage", "dp", None, None, "tp")

    def device_step(act_in, w_conv, w_short, gamma, beta, gamma_s, grad_z):
        any_spec = pl.BlockSpec(memory_space=pl.ANY)
        vm_spec = pl.BlockSpec(memory_space=pltpu.VMEM)
        dma = pltpu.SemaphoreType.DMA
        sds = jax.ShapeDtypeStruct
        z_shape, dx_shape = sds((IMAGES, SIDE, SIDE, LANES), BF), sds((3, SIDE, SIDE, CHANNELS), BF)
        block = [pltpu.VMEM((8 * HALO + WIDE, LANES), BF), pltpu.VMEM((UNIT, LANES), BF)]
        mids = pl.pallas_call(
            block_kernel,
            out_shape=(
                z_shape,
                dx_shape,
                sds((10, LANES, CHANNELS), F32),
                sds((3, LANES, UNIT), BF),
                sds((PARTS, UNIT, LANES), BF),
                sds((PARTS, 1, LANES), F32),
                sds((PARTS, 1, LANES), F32),
            ),
            in_specs=[any_spec] * 5 + [vm_spec, any_spec],
            out_specs=(any_spec,) * 7,
            scratch_shapes=[
                pltpu.VMEM((IMAGES * HALO + WIDE, CHANNELS), BF),
                pltpu.VMEM((10, LANES, CHANNELS), BF),
                pltpu.VMEM((10, CHANNELS, LANES), BF),
                pltpu.VMEM((PARTS, 1, LANES), F32),
                pltpu.VMEM((PARTS, 1, LANES), F32),
                pltpu.VMEM((IMAGES * ROWS, LANES), BF),
                pltpu.VMEM((2, PARTS, IMAGES * ROWS, LANES), BF),
                pltpu.VMEM((IMAGES * ROWS, LANES), BF),
                pltpu.VMEM((3, LANES, 24 * ROWS), BF),
                *block,
                *block,
                pltpu.VMEM((PARTS * HALO + WIDE, CHANNELS), BF),
                pltpu.VMEM((PARTS * ROWS, CHANNELS), BF),
                pltpu.VMEM((10, LANES, CHANNELS), F32),
                pltpu.VMEM((IMAGES, SIDE, SIDE, LANES), BF),
                pltpu.VMEM((IMAGES, SIDE, SIDE, LANES), BF),
                dma((100,)),
                dma((20,)),
                dma((2, 2, 3)),
                dma((2,)),
                dma((2, 5)),
                dma((2, 5)),
                dma((3, 2)),
                dma((IMAGES,)),
                dma((IMAGES, 2)),
                dma((3, PARTS)),
                dma((2, PARTS, 3)),
                dma((3, PARTS)),
                dma((3, PARTS)),
                dma((3, 2)),
            ],
            compiler_params=pltpu.CompilerParams(has_side_effects=True, collective_id=0, vmem_limit_bytes=67043328),
        )(act_in[0], w_conv[0].reshape(TAPS, LANES, CHANNELS), w_short[0], gamma, gamma_s, beta, grad_z[0])
        z, dx, dw, ds = pl.pallas_call(
            last_kernel,
            out_shape=(z_shape, dx_shape, sds((TAPS, LANES, CHANNELS), F32), sds((LANES, CHANNELS), F32)),
            in_specs=[any_spec] * 5 + [vm_spec] * 2,
            out_specs=(any_spec,) * PARTS,
            scratch_shapes=[
                pltpu.VMEM((3, LANES, UNIT), BF),
                pltpu.VMEM((PARTS, UNIT, LANES), BF),
                *block,
                *block,
                pltpu.VMEM((PARTS, 10, LANES, LANES), F32),
                pltpu.VMEM((IMAGES, SIDE, SIDE, LANES), BF),
                pltpu.VMEM((3, SIDE, SIDE, CHANNELS), BF),
                dma((24,)),
            ],
            compiler_params=pltpu.CompilerParams(vmem_limit_bytes=67043328),
        )(*mids)
        return z[None], dx[None], dw.reshape(1, 3, 3, LANES, CHANNELS), ds[None]

    return jax.shard_map(device_step, mesh=mesh, in_specs=(act_spec, kernel_spec, short_spec, vec_spec, vec_spec, vec_spec, grad_spec), out_specs=(grad_spec, act_spec, kernel_spec, short_spec), check_vma=False)
```

```python
import jax
import jax.numpy as jnp
from jax import lax
from jax.experimental import pallas as pl
from jax.experimental.pallas import tpu as pltpu
from jax.sharding import PartitionSpec as P

BF = jnp.bfloat16
F32 = jnp.float32
MESH = pl.DeviceIdType.MESH
PARTS = 4
LANES = 256
CHANNELS = 1024
WIDE = 16
SIDE = 14
TAPS = 9
IMAGES = 12
PAIR = 448
ROWS = 224
HALO = 240
SET = 4 * ROWS
UNIT = 8 * ROWS
NT = (((1,), (1,)), ((), ()))


def dot(a, b):
    return jnp.dot(a, b, preferred_element_type=F32)


def dot_t(a, b):
    return lax.dot_general(a, b, NT, preferred_element_type=F32)


def mo(v, m):
    return pl.multiple_of(v, m)


def zcols(q):
    return pl.ds(mo(q * LANES, LANES), LANES)


def scale_block(value, gam, gsc, gh, gsh):
    for n in range(8):
        v = value(n).astype(F32)
        gh[n * HALO + WIDE:n * HALO + HALO] = (v * gam).astype(BF)
        gsh[n * ROWS:n * ROWS + ROWS] = (v * gsc).astype(BF)


def weight_dots(xt, lanes, gh, gsh, put):
    for i in range(3):
        rhs = jnp.concatenate([gh[n * HALO + (2 - i) * WIDE:n * HALO + (2 - i) * WIDE + ROWS] for n in range(8)], axis=0)
        for j in range(3):
            put(3 * i + j, dot(xt[j, :, lanes], rhs))
    put(TAPS, dot(xt[1, :, lanes], gsh[...]))


def block_kernel(
    act, wc, ws, gam_in, gs_in, bet, dz_in,
    z_out, dx_out, acc_out, xt_out, g_out, gam_out, gs_out,
    xa, wo, wr, gamv, gsv, dz, ga, xz, xt, gh0, gsh0, gh1, gsh1, gx, gsx, dwa, zs, dxs,
    s_send, s_loc, s_tail, r_ws, r_wx, r_wz, r_v, r_x, r_xs, r_xz, r_g, r_dx, r_rel, r_h,
):
    z = lax.axis_index("dp")
    st = lax.axis_index("stage")
    k = lax.axis_index("tp")
    zo = 1 - z
    k1 = k + 1 - 2 * lax.rem(k, 2)
    k2 = lax.rem(k + 2, PARTS)
    k3 = 3 - k
    kx = k // 2
    qa = 2 * kx
    kc = mo(k * LANES, LANES)

    def dev(dp=None, stage=None, tp=None):
        return (z if dp is None else dp, st if stage is None else stage, k if tp is None else tp)

    sends = []

    def remote(src, dst, ssem, rsem, **to):
        return pltpu.make_async_remote_copy(src, dst, ssem, rsem, device_id=dev(**to), device_id_type=MESH)

    def send(src, dst, rsem, **to):
        c = remote(src, dst, s_send.at[len(sends)], rsem, **to)
        c.start()
        sends.append(c)

    def recv(dst, rsem):
        remote(dst, dst, s_send.at[0], rsem).wait_recv()

    def image(i, j):
        return xa.at[pl.ds(mo(((i * PARTS + j) * 15 + 1) * WIDE, WIDE), ROWS)]

    def img_rows(i, j):
        return pl.ds(mo((i * PARTS + j) * ROWS, 32), ROWS)

    barrier = pltpu.get_barrier_semaphore()

    def greet(peers):
        for p in peers:
            pl.semaphore_signal(barrier, inc=1, device_id=dev(**p), device_id_type=MESH)
        pl.semaphore_wait(barrier, len(peers))

    @pl.when(st == 0)
    def _():
        loads = [
            pltpu.make_async_copy(act.at[i, :, :, zcols(q)], zs.at[i * PARTS + q], s_loc.at[i * PARTS + q])
            for i in range(3) for q in range(PARTS)
        ]
        for c in loads:
            c.start()
        greet([dict(tp=k2), dict(dp=zo), dict(stage=1, tp=qa), dict(stage=1, tp=qa + 1)])

        def to_z(i, j):
            for n in range(2):
                src = xa.at[pl.ds(mo(((i * PARTS + j) * 15 + 1) * WIDE, WIDE), ROWS), zcols(qa + n)]
                send(src, ga.at[0, qa + n, img_rows(i, j)], r_xs.at[i * PARTS + j, n], dp=zo)

        def y_image(i, j):
            send(image(i, j), image(i, j), r_x.at[i * PARTS + j], stage=1)

        def x_image(i):
            send(image(i, k), image(i, k), r_x.at[i * PARTS + k], tp=k2)

        for i in range(3):
            for c in loads[PARTS * i:PARTS * i + PARTS]:
                c.wait()

            def pad(h, _):
                rows = pl.ds(mo(((i * PARTS + k) * 15 + 1 + h) * WIDE, WIDE), WIDE)
                for q in range(PARTS):
                    xa[rows, q * LANES:q * LANES + LANES] = jnp.concatenate([zs[i * PARTS + q, h], jnp.zeros((2, LANES), BF)], axis=0)
                return 0

            lax.fori_loop(0, SIDE, pad, 0)
            if i == 0:
                x_image(0)
                y_image(0, k)
            if i == 1:
                y_image(1, k)
        x_image(2)
        x_image(1)
        for i in range(3):
            to_z(i, k)
        recv(image(0, k2), r_x.at[k2])
        y_image(0, k2)
        y_image(2, k)
        recv(image(2, k2), r_x.at[8 + k2])
        y_image(2, k2)
        recv(image(1, k2), r_x.at[PARTS + k2])
        for i in range(3):
            to_z(i, k2)
        for i in range(3):
            for j in (k, k2):
                for n in range(2):
                    buf = ga.at[0, qa + n, img_rows(i, j)]
                    recv(buf, r_xs.at[i * PARTS + j, n])
                    send(buf, xz.at[img_rows(i, j)], r_xz.at[i, j], stage=1, tp=qa + n)
        zs[...] = jnp.zeros((IMAGES, SIDE, SIDE, LANES), BF)
        fill = pltpu.make_async_copy(zs, z_out, s_loc.at[0])
        fill.start()
        fill.wait()
        for i in range(3):
            for n in range(2):
                q = qa + n
                recv(dxs.at[i * PARTS + q], r_rel.at[i, q])
                send(dxs.at[i * PARTS + q], dx_out.at[i, :, :, zcols(q)], r_dx.at[i, q], tp=k2)
        for i in range(3):
            for q in range(PARTS):
                recv(dx_out.at[i, :, :, zcols(q)], r_dx.at[i, q])
        for c in sends:
            c.wait_send()

    sends.clear()

    @pl.when(st == 1)
    def _():
        local = [
            pltpu.make_async_copy(dz_in, zs, s_loc.at[0]),
            pltpu.make_async_copy(gam_in, gamv.at[k], s_loc.at[1]),
            pltpu.make_async_copy(gs_in, gsv.at[k], s_loc.at[2]),
            pltpu.make_async_copy(wc.at[:, :, pl.ds(kc, LANES)], wr.at[pl.ds(0, TAPS), pl.ds(kc, LANES)], s_loc.at[3]),
            pltpu.make_async_copy(ws.at[:, pl.ds(kc, LANES)], wr.at[TAPS, pl.ds(kc, LANES)], s_loc.at[PARTS]),
            pltpu.make_async_copy(wc, wo.at[pl.ds(0, TAPS)], s_loc.at[5]),
            pltpu.make_async_copy(ws, wo.at[TAPS], s_loc.at[6]),
        ]
        for c in local:
            c.start()

        def zero_rows(n, _):
            xa[pl.ds(mo(n * HALO, WIDE), WIDE)] = jnp.zeros((WIDE, CHANNELS), BF)
            return 0

        lax.fori_loop(0, 13, zero_rows, 0)
        greet([dict(tp=k1), dict(tp=k2), dict(tp=k3), dict(dp=zo), dict(stage=0, tp=qa), dict(stage=0, tp=qa + 1)])

        def wdst(tap, q):
            return wr.at[tap, zcols(q)]

        mine, other = z * 5, zo * 5

        def wsend(t, q, n):
            ssem, rsem = s_send.at[len(sends)], r_wx.at[n, t]
            if t < PARTS:
                send(wc.at[mine + t, :, zcols(q)], wdst(mine + t, k), rsem, tp=q)
                return

            @pl.when(z == 0)
            def _():
                remote(wc.at[PARTS, :, zcols(q)], wdst(PARTS, k), ssem, rsem, tp=q).start()

            @pl.when(z == 1)
            def _():
                remote(ws.at[:, zcols(q)], wdst(TAPS, k), ssem, rsem, tp=q).start()

            sends.append(remote(ws.at[:, zcols(q)], wdst(TAPS, k), ssem, rsem, tp=q))

        for n, p in enumerate((k1, k2, k3)):
            send(gam_in, gamv.at[k], r_v.at[n, 0], tp=p)
            send(gs_in, gsv.at[k], r_v.at[n, 1], tp=p)
        for t in range(5):
            wsend(t, k2, 0)
            wsend(t, k3, 1)
        send(wc.at[:, :, zcols(k1)], wr.at[pl.ds(0, TAPS), pl.ds(kc, LANES)], r_ws.at[0], tp=k1)
        send(ws.at[:, zcols(k1)], wr.at[TAPS, pl.ds(kc, LANES)], r_ws.at[1], tp=k1)
        def set_up():
            for n in range(5):
                gx[pl.ds(n * HALO, WIDE)] = jnp.zeros((WIDE, CHANNELS), BF)
            for n in range(TAPS):
                gh0[pl.ds(n * HALO, WIDE)] = jnp.zeros((WIDE, LANES), BF)
                gh1[pl.ds(n * HALO, WIDE)] = jnp.zeros((WIDE, LANES), BF)
            dxs[0:3] = jnp.zeros((3, SIDE, SIDE, LANES), BF)
            for c in local:
                c.wait()
            for c in fills:
                c.start()

        fills = [
            pltpu.make_async_copy(dxs.at[pl.ds(0, 3)], dx_out.at[:, :, :, zcols(q)], s_loc.at[10 + q]) for q in range(PARTS)
        ]

        def pad_dz(n, _):
            row = (lax.rem(n, 3) * PARTS + n // 3) * ROWS
            for h in range(SIDE):
                dz[pl.ds(mo(row + h * WIDE, WIDE), WIDE)] = jnp.concatenate([zs[n, h], jnp.zeros((2, LANES), BF)], axis=0)
            return 0

        def take(i, j):
            recv(image(i, j), r_x.at[i * PARTS + j])

        def pass_on(i, j, tp):
            send(image(i, j), image(i, j), r_x.at[i * PARTS + j], tp=tp)

        def fwd(i, b, mode):
            gam, beta, gsc = gamv[k], bet[...], gsv[k]
            bases = [mo((i * PARTS + b * 2 + n) * HALO, WIDE) for n in range(2)]
            ch = {
                "all": pl.ds(0, CHANNELS),
                "own": pl.ds(mo(kx * 512, 512), 512),
                "rest": pl.ds(mo((1 - kx) * 512, 512), 512),
            }[mode]

            def lhs(t):
                return jnp.concatenate([xa[pl.ds(mo(s + t * WIDE, WIDE), ROWS), ch] for s in bases], axis=0)

            parts = []
            for j in range(3):
                acc = dot(lhs(0), wr[j, ch])
                acc += dot(lhs(1), wr[3 + j, ch])
                acc += dot(lhs(2), wr[6 + j, ch])
                parts.append(acc)
            pre = parts[1] + pltpu.roll(parts[0], 1, 0) + pltpu.roll(parts[2], 447, 0)
            u = pre * gam + dot(lhs(1), wr[TAPS, ch]) * gsc
            if mode == "own":
                for n in range(2):
                    dwa[b * 2 + n, 0:ROWS, i * LANES:i * LANES + LANES] = u[n * ROWS:n * ROWS + ROWS]
                return
            if mode == "rest":
                u += jnp.concatenate([dwa[b * 2 + n, 0:ROWS, i * LANES:i * LANES + LANES] for n in range(2)], axis=0)
            u += beta
            at = pl.ds(mo(i * SET + b * PAIR, 64), PAIR)
            zb = jnp.maximum(u, 0.0).astype(BF)
            for n in range(2):
                for h in range(SIDE):
                    zs[(b * 2 + n) * 3 + i, h] = zb[(n * SIDE + h) * WIDE:(n * SIDE + h) * WIDE + SIDE]
            ga[z, k, at] = jnp.where(u > 0.0, dz[at].astype(F32), 0.0).astype(BF)

        def fwd_set(i, mode):
            def body(b, _):
                fwd(i, b, mode)
                return 0

            lax.fori_loop(0, 2, body, 0)

        def blk(zz, q, i):
            return ga.at[zz, q, pl.ds(mo(i * SET, 128), SET)]

        def gsend(zz, q, i, **to):
            send(blk(zz, q, i), blk(zz, q, i), r_g.at[zz, q, i], **to)

        def grecv(zz, q, i):
            recv(blk(zz, q, i), r_g.at[zz, q, i])

        def put_xt(val, t):
            v = val.astype(F32)
            for j in range(3):
                w = v if j == 1 else pltpu.roll(v, (1 - j) % SET, 0)
                xt[j, :, pl.ds(t * SET, SET)] = w.T.astype(BF)

        def dx(i, n0):
            for q in range(PARTS):
                gam, gsc = gamv[q], gsv[q]

                def scale(n, _):
                    v = ga[z, q, pl.ds(mo(i * SET + n * ROWS, 32), ROWS)].astype(F32)
                    gx[pl.ds(mo(n * HALO + WIDE, WIDE), ROWS), pl.ds(q * LANES, LANES)] = (v * gam).astype(BF)
                    gsx[pl.ds(mo(n * ROWS, 32), ROWS), pl.ds(q * LANES, LANES)] = (v * gsc).astype(BF)
                    return 0

                lax.fori_loop(0, PARTS, scale, 0)

            def body(b):
                bases = [mo((b * 2 + n) * HALO, WIDE) for n in range(2)]

                def lhs(t):
                    return jnp.concatenate([gx[pl.ds(mo(s + (2 - t) * WIDE, WIDE), ROWS)] for s in bases], axis=0)

                parts = []
                for j in range(3):
                    acc = dot_t(lhs(0), wo[j])
                    acc += dot_t(lhs(1), wo[3 + j])
                    acc += dot_t(lhs(2), wo[6 + j])
                    parts.append(acc)
                tot = parts[1] + pltpu.roll(parts[0], 447, 0) + pltpu.roll(parts[2], 1, 0)
                tot += dot_t(gsx[pl.ds(mo(b * PAIR, 64), PAIR)], wo[TAPS])
                db = tot.astype(BF)
                for n in range(2):
                    for h in range(SIDE):
                        dxs[i * PARTS + b * 2 + n, h] = db[(n * SIDE + h) * WIDE:(n * SIDE + h) * WIDE + SIDE]

            def step(m, _):
                body(jnp.where(m == 0, 1 - kx, kx))

                @pl.when(m == 0)
                def _():
                    for j, via, ssem in out[0]:
                        remote(dxs.at[i * PARTS + j], dxs.at[i * PARTS + k], ssem, r_rel.at[i, k], stage=0, tp=via).start()

                @pl.when(m == 1)
                def _():
                    for j, via, ssem in out[1]:
                        remote(
                            dxs.at[i * PARTS + j], dx_out.at[i, :, :, pl.ds(kc, LANES)], ssem, r_dx.at[i, k], stage=0, tp=via
                        ).start()

                return 0

            out = (
                ((k2, k, s_send.at[n0]), (k3, k1, s_send.at[n0 + 1])),
                ((k, k, s_send.at[n0 + 2]), (k1, k1, s_send.at[n0 + 3])),
            )
            lax.fori_loop(0, 2, step, 0)

        def dx_sends(count):
            n0 = len(sends)
            for n in range(PARTS * count):
                sends.append(remote(dxs.at[0], dxs.at[0], s_send.at[n0 + n], r_rel.at[0, 0]))
            return n0

        def quarter(n):
            b = lax.rem(k + 2 * (n // 2), PARTS)
            return b + lax.rem(n, 2) * (1 - 2 * lax.rem(b, 2))

        def dw(u, first, lo, hi):
            bufs = ((gh0, gsh0), (gh1, gsh1))

            def scale(n, m):
                q = quarter(n)

                def value(r):
                    t = u * 8 + r
                    zz = z if t < IMAGES else zo
                    return ga[zz, q, pl.ds((t % IMAGES) * ROWS, ROWS)]

                scale_block(value, gamv[q], gsv[q], *bufs[m])

            def pair(half, _):
                for m in range(2):
                    n = 2 * half + m
                    cols = zcols(quarter(n))

                    def put(tap, d):
                        if first:
                            dwa[tap, :, cols] = d
                        else:
                            dwa[tap, :, cols] += d

                    if m == 0:
                        scale(n + 1, 1)
                    elif hi - lo > 1:
                        scale(jnp.minimum(n + 1, 3), 0)
                    weight_dots(xt, pl.ds(u * UNIT, UNIT), *bufs[m], put)
                    if not first:
                        pltpu.make_async_copy(dwa.at[:, :, cols], acc_out.at[:, :, cols], s_loc.at[10 + n]).start()
                return 0

            scale(2 * lo, 0)
            lax.fori_loop(lo, hi, pair, 0)

        def collect(i):
            take(i, k1)
            take(i, k3)

        def spread(i):
            gsend(z, k, i, tp=k2)
            gsend(z, k, i, dp=zo)
            gsend(z, k, i, tp=k1)
            put_xt(
                jnp.concatenate(
                    [xa[pl.ds(((i * PARTS + j) * 15 + 1) * WIDE, ROWS), pl.ds(kc, LANES)] for j in range(PARTS)], axis=0
                ),
                i,
            )

        def relay_x(i):
            grecv(z, k2, i)
            gsend(z, k2, i, tp=k1)

        def relay_z(i):
            grecv(zo, k, i)
            gsend(zo, k, i, tp=k1)

        def half(zz, q, h):
            return ga.at[zz, q, pl.ds(2 * SET + h * PAIR, PAIR)]

        def diagonal(i):
            if i == 0:
                gsend(zo, k, 0, tp=k2)
            if i == 1:
                gsend(z, k2, 1, dp=zo)
            if i == 2:
                send(half(zo, k, 0), half(zo, k, 0), r_h.at[0], tp=k2)
                send(half(z, k2, 1), half(z, k2, 1), r_h.at[1], dp=zo)

        def diagonal_recv(i):
            if i == 2:
                recv(half(zo, k2, 0), r_h.at[0])
                recv(half(zo, k2, 1), r_h.at[1])
            else:
                grecv(zo, k2, i)
            gsend(zo, k2, i, tp=k1)

        for t in range(5):
            for s, q in ((0, k2), (1, k3)):
                recv(wdst(mine + t, q), r_wx.at[s, t])
                send(wdst(mine + t, q), wdst(mine + t, q), r_wz.at[s, t], dp=zo)
            if t == 0:
                set_up()
                for n, p in enumerate((k1, k2, k3)):
                    recv(gamv.at[p], r_v.at[n, 0])
                    recv(gsv.at[p], r_v.at[n, 1])
                recv(wr.at[pl.ds(0, TAPS), zcols(k1)], r_ws.at[0])
                recv(wr.at[TAPS, zcols(k1)], r_ws.at[1])
            if t == 1:
                lax.fori_loop(0, IMAGES, pad_dz, 0)
                take(0, k)
                pass_on(0, k, k1)
            if t == 2:
                for c in fills:
                    c.wait()
                take(0, k1)
                fwd(0, kx, "own")
            if t == 3:
                take(1, k)
                pass_on(1, k, k2)
                pass_on(1, k, k1)
        take(1, k1)
        fwd(1, kx, "own")
        take(0, k2)
        pass_on(0, k2, k1)
        take(0, k3)
        fwd(0, 1 - kx, "own")
        for t in range(5):
            for s, q in ((0, k2), (1, k3)):
                recv(wdst(other + t, q), r_wz.at[s, t])
        fwd_set(0, "rest")
        spread(0)
        fwd(1, kx, "rest")
        take(1, k2)
        pass_on(1, k2, k1)
        take(2, k)
        pass_on(2, k, k1)
        take(1, k3)
        fwd(1, 1 - kx, "all")
        spread(1)
        grecv(z, k1, 0)
        grecv(z, k1, 1)
        dw(0, True, 0, 1)
        relay_z(0)
        relay_x(0)
        take(2, k2)
        pass_on(2, k2, k1)
        collect(2)
        fwd_set(2, "all")
        spread(2)
        zcopy = pltpu.make_async_copy(zs, z_out, s_loc.at[8])
        zcopy.start()
        diagonal(0)
        relay_x(1)
        diagonal(1)
        relay_z(1)
        n01 = dx_sends(2)

        def dx01(i, _):
            grecv(z, k3, i)
            dx(i, n01 + PARTS * i)
            return 0

        lax.fori_loop(0, 2, dx01, 0)
        relay_x(2)
        relay_z(2)
        diagonal(2)
        dw(0, True, 1, 2)
        grecv(z, k1, 2)
        grecv(z, k3, 2)
        dx(2, dx_sends(1))
        copies = [
            pltpu.make_async_copy(gamv, gam_out, s_loc.at[6]),
            pltpu.make_async_copy(gsv, gs_out, s_loc.at[7]),
        ]
        for c in copies:
            c.start()
        tail = []

        def leave(src, dst):
            c = pltpu.make_async_copy(src, dst, s_tail.at[len(tail)])
            c.start()
            tail.append(c)

        def arrive(i):
            diagonal_recv(i)
            for j in range(PARTS):
                recv(xz.at[pl.ds(i * SET + j * ROWS, ROWS)], r_xz.at[i, j])
            put_xt(xz[pl.ds(i * SET, SET)], 3 + i)

        def leave_early(i):
            at = pl.ds((i - 1) * SET, SET)
            leave(xt.at[:, :, pl.ds((3 + i) * SET, SET)], xt_out.at[:, :, at])
            for q in (k, k2):
                leave(blk(zo, q, i), g_out.at[q, at])

        arrive(0)
        arrive(1)
        leave_early(1)
        grecv(zo, k1, 0)
        grecv(zo, k3, 0)
        dw(1, False, 0, 2)
        arrive(2)
        leave_early(2)
        for i in (1, 2):
            at = pl.ds((i - 1) * SET, SET)
            grecv(zo, k1, i)
            grecv(zo, k3, i)
            for q in (k1, k3):
                leave(blk(zo, q, i), g_out.at[q, at])
        for c in tail + copies + [zcopy]:
            c.wait()
        for n in range(PARTS):
            cols = zcols(quarter(n))
            pltpu.make_async_copy(dwa.at[:, :, cols], acc_out.at[:, :, cols], s_loc.at[10 + n]).wait()
        for c in sends:
            c.wait_send()


def last_kernel(
    z_in, dx_in, acc, xt_in, g_in, gamv, gsv,
    z_out, dx_out, dw_out, ds_out,
    xt, g, gh0, gsh0, gh1, gsh1, dwa, zb, dxb,
    sem,
):
    st = lax.axis_index("stage")
    bounce = [
        (pltpu.make_async_copy(z_in, zb, sem.at[0]), pltpu.make_async_copy(zb, z_out, sem.at[1])),
        (pltpu.make_async_copy(dx_in, dxb, sem.at[2]), pltpu.make_async_copy(dxb, dx_out, sem.at[3])),
    ]

    def outs(q):
        cols = zcols(q)
        return (
            pltpu.make_async_copy(dwa.at[q, pl.ds(0, TAPS)], dw_out.at[:, :, cols], sem.at[PARTS + 2 * q]),
            pltpu.make_async_copy(dwa.at[q, TAPS], ds_out.at[:, cols], sem.at[5 + 2 * q]),
        )

    @pl.when(st == 0)
    def _():
        for c, _n in bounce:
            c.start()

        def zero(tap, _):
            for q in range(PARTS):
                dwa[q, tap] = jnp.zeros((LANES, LANES), F32)
            return 0

        lax.fori_loop(0, 10, zero, 0)
        for q in range(PARTS):
            for c in outs(q):
                c.start()
        for c, n in bounce:
            c.wait()
            n.start()
        for _c, n in bounce:
            n.wait()
        for q in range(PARTS):
            for c in outs(q):
                c.wait()

    @pl.when(st == 1)
    def _():
        loads = [pltpu.make_async_copy(g_in.at[0], g.at[0], sem.at[IMAGES])]
        loads += [pltpu.make_async_copy(xt_in.at[j], xt.at[j], sem.at[WIDE + j]) for j in range(3)]
        accs = [pltpu.make_async_copy(acc.at[:, :, zcols(q)], dwa.at[q], sem.at[20 + q]) for q in range(PARTS)]
        more = [pltpu.make_async_copy(g_in.at[q], g.at[q], sem.at[IMAGES + q]) for q in range(1, PARTS)]
        for c in [*loads, accs[0], more[0], accs[1], *more[1:], *accs[2:]]:
            c.start()
        for c, _n in bounce:
            c.start()
        for n in range(TAPS):
            gh0[pl.ds(n * HALO, WIDE)] = jnp.zeros((WIDE, LANES), BF)
            gh1[pl.ds(n * HALO, WIDE)] = jnp.zeros((WIDE, LANES), BF)
        bufs = ((gh0, gsh0), (gh1, gsh1))

        def scale(q, m):
            def value(n):
                return g[q, pl.ds(n * ROWS, ROWS)]

            scale_block(value, gamv[q], gsv[q], *bufs[m])

        loads[0].wait()
        scale(0, 0)
        for c in loads[1:]:
            c.wait()

        def pair(half, _):
            @pl.when(half == 1)
            def _():
                for c, n in bounce:
                    c.wait()
                    n.start()

            for m in range(2):
                q = 2 * half + m
                pltpu.make_async_copy(acc.at[:, :, zcols(q)], dwa.at[q], sem.at[20 + q]).wait()
                after = jnp.minimum(q + 1, 3)

                @pl.when(q < 3)
                def _():
                    pltpu.make_async_copy(g_in.at[after], g.at[after], sem.at[IMAGES + after]).wait()

                scale(after, 1 - m)

                def put(tap, d):
                    dwa[q, tap] += d

                weight_dots(xt, pl.ds(0, UNIT), *bufs[m], put)
                for c in outs(q):
                    c.start()
            return 0

        lax.fori_loop(0, 2, pair, 0)
        for _c, n in bounce:
            n.wait()
        for q in range(PARTS):
            for c in outs(q):
                c.wait()


def solution(mesh):
    act_spec = P("stage", ("dp", "tp"), None, None, None)
    kernel_spec = P("stage", None, None, "tp", None)
    short_spec = P("stage", "tp", None)
    vec_spec = P("stage", "tp")
    grad_spec = P("stage", "dp", None, None, "tp")

    def device_step(act_in, w_conv, w_short, gamma, beta, gamma_s, grad_z):
        any_spec = pl.BlockSpec(memory_space=pl.ANY)
        vm_spec = pl.BlockSpec(memory_space=pltpu.VMEM)
        dma = pltpu.SemaphoreType.DMA
        sds = jax.ShapeDtypeStruct
        z_shape, dx_shape = sds((IMAGES, SIDE, SIDE, LANES), BF), sds((3, SIDE, SIDE, CHANNELS), BF)
        block = [pltpu.VMEM((8 * HALO + WIDE, LANES), BF), pltpu.VMEM((UNIT, LANES), BF)]
        mids = pl.pallas_call(
            block_kernel,
            out_shape=(
                z_shape,
                dx_shape,
                sds((10, LANES, CHANNELS), F32),
                sds((3, LANES, UNIT), BF),
                sds((PARTS, UNIT, LANES), BF),
                sds((PARTS, 1, LANES), F32),
                sds((PARTS, 1, LANES), F32),
            ),
            in_specs=[any_spec] * 5 + [vm_spec, any_spec],
            out_specs=(any_spec,) * 7,
            scratch_shapes=[
                pltpu.VMEM((IMAGES * HALO + WIDE, CHANNELS), BF),
                pltpu.VMEM((10, LANES, CHANNELS), BF),
                pltpu.VMEM((10, CHANNELS, LANES), BF),
                pltpu.VMEM((PARTS, 1, LANES), F32),
                pltpu.VMEM((PARTS, 1, LANES), F32),
                pltpu.VMEM((IMAGES * ROWS, LANES), BF),
                pltpu.VMEM((2, PARTS, IMAGES * ROWS, LANES), BF),
                pltpu.VMEM((IMAGES * ROWS, LANES), BF),
                pltpu.VMEM((3, LANES, 24 * ROWS), BF),
                *block,
                *block,
                pltpu.VMEM((PARTS * HALO + WIDE, CHANNELS), BF),
                pltpu.VMEM((PARTS * ROWS, CHANNELS), BF),
                pltpu.VMEM((10, LANES, CHANNELS), F32),
                pltpu.VMEM((IMAGES, SIDE, SIDE, LANES), BF),
                pltpu.VMEM((IMAGES, SIDE, SIDE, LANES), BF),
                dma((100,)),
                dma((20,)),
                dma((10,)),
                dma((2,)),
                dma((2, 5)),
                dma((2, 5)),
                dma((3, 2)),
                dma((IMAGES,)),
                dma((IMAGES, 2)),
                dma((3, PARTS)),
                dma((2, PARTS, 3)),
                dma((3, PARTS)),
                dma((3, PARTS)),
                dma((2,)),
            ],
            compiler_params=pltpu.CompilerParams(has_side_effects=True, collective_id=0, vmem_limit_bytes=67043328),
        )(act_in[0], w_conv[0].reshape(TAPS, LANES, CHANNELS), w_short[0], gamma, gamma_s, beta, grad_z[0])
        z, dx, dw, ds = pl.pallas_call(
            last_kernel,
            out_shape=(z_shape, dx_shape, sds((TAPS, LANES, CHANNELS), F32), sds((LANES, CHANNELS), F32)),
            in_specs=[any_spec] * 5 + [vm_spec] * 2,
            out_specs=(any_spec,) * PARTS,
            scratch_shapes=[
                pltpu.VMEM((3, LANES, UNIT), BF),
                pltpu.VMEM((PARTS, UNIT, LANES), BF),
                *block,
                *block,
                pltpu.VMEM((PARTS, 10, LANES, LANES), F32),
                pltpu.VMEM((IMAGES, SIDE, SIDE, LANES), BF),
                pltpu.VMEM((3, SIDE, SIDE, CHANNELS), BF),
                dma((24,)),
            ],
            compiler_params=pltpu.CompilerParams(vmem_limit_bytes=67043328),
        )(*mids)
        return z[None], dx[None], dw.reshape(1, 3, 3, LANES, CHANNELS), ds[None]

    return jax.shard_map(device_step, mesh=mesh, in_specs=(act_spec, kernel_spec, short_spec, vec_spec, vec_spec, vec_spec, grad_spec), out_specs=(grad_spec, act_spec, kernel_spec, short_spec), check_vma=False)
```
